32 devices in a mesh: groups: 2 (over y), seq: 4 (over z), heads: 2 (over x), sub: 2 (over core).
Axes of the slice: x: 2, y: 2, z: 4, core: 2. Of those that a mesh axis runs over, the one named last changes fastest.
Arguments:
- queries: bfloat16 [2048, 8192], P(('groups', 'seq', 'sub'), 'heads'), parts along dimension 0, may hold values from -400 to 400
- keys: bfloat16 [2048, 1024], P(('groups', 'seq', 'sub'), 'heads'), parts along dimension 0, may hold values from -6 to 6
- values: bfloat16 [2048, 1024], P(('groups', 'seq', 'sub'), 'heads'), parts along dimension 0, may hold values from -18 to 18
- half_order: int32 [32], P('groups'), parts along dimension 0, may hold values from 0 to 15, as said below
- frame_lengths: int32 [16], P('groups'), parts along dimension 0, may hold values from 1 to 256, 1024 in all
- out_proj: bfloat16 [8192, 4096], P('heads', ('seq', 'sub')), may hold values from -0.09375 to 0.09375
- residual_in: bfloat16 [2048, 4096], P(('groups', 'seq', 'sub'), 'heads'), parts along dimension 0, may hold values from -40 to 40
- norm_gain: float32 [4096], P('heads'), may hold values from 0.5 to 1.5
Outputs:
- attended: bfloat16 [2048, 8192], P(('groups', 'seq', 'sub'), 'heads'), parts along dimension 0
- hidden_state: bfloat16 [2048, 4096], P(('groups', 'seq', 'sub'), 'heads'), parts along dimension 0
- normed: bfloat16 [2048, 4096], P(('groups', 'seq', 'sub'), 'heads'), parts along dimension 0
The draws below stay inside these ranges and needn't reach their ends.
There are 2 independent parts, one for each index of `groups`. The reference program is written for one: setup_inputs(seed, part) draws one part's arguments, and reference() takes and returns one part's arrays. A program takes and returns all parts, laid end to end along the dimension named above; an argument that names none is the same for every part. Nothing has to cross between parts.
Inputs may be any that keep to these rules, and one draw needn't show every extreme that they name: `half_order`: a permutation of 0 to 15.
All inputs are finite; a program needn't handle non-finite values.
Results may differ from the reference program's by a relative error of at most 0.005.
Values may be sent and summed in bfloat16 or wider, within the bound.
A program may use at most 128 MiB of HBM per device.

```python
import math
import jax
import jax.numpy as jnp
import numpy as np
from jax import lax

QUERY_HEAD_COUNT = 64
KEY_VALUE_HEADS = 8
HEAD_WIDTH = 128
OUT_WIDTH = 4096
CLIP_TOKENS = 1024
HALF = 64
HALVES = 16
FRAMES = 8
FRAME_MOST = 256


def order_table(key):
    return jax.random.permutation(jax.random.fold_in(key, 11), HALVES).astype(jnp.int32)


def draw_half_order(key, part):
    return order_table(key)


def draw_keys(key, part):
    filled_rows = jax.random.normal(jax.random.fold_in(key, 17), (CLIP_TOKENS, KEY_VALUE_HEADS * HEAD_WIDTH), jnp.float32)
    return jnp.clip(filled_rows, -6.0, 6.0).astype(jnp.bfloat16)


def draw_queries(key, part):
    filled_rows = 1.5 * jax.random.normal(jax.random.fold_in(key, 31), (CLIP_TOKENS, QUERY_HEAD_COUNT * HEAD_WIDTH), jnp.float32)
    return jnp.clip(filled_rows, -400.0, 400.0).astype(jnp.bfloat16)


def draw_residual_in(key, part):
    column_base = jnp.exp(math.log(4.0) * jnp.arange(OUT_WIDTH, dtype=jnp.float32) / OUT_WIDTH) * 0.5
    column_jitter = jnp.exp(jax.random.uniform(jax.random.fold_in(key, 41), (OUT_WIDTH,), jnp.float32, math.log(0.7), math.log(1.4)))
    entries = jax.random.normal(jax.random.fold_in(key, 43), (CLIP_TOKENS, OUT_WIDTH), jnp.float32)
    row_scale = jnp.exp(jax.random.uniform(jax.random.fold_in(key, 47), (CLIP_TOKENS,), jnp.float32, 0.0, math.log(10.0)))
    filled_rows = entries * (column_base * column_jitter)[None, :] * row_scale[:, None]
    return jnp.clip(filled_rows, -40.0, 40.0).astype(jnp.bfloat16)


def strengthened(values, key, source, target, parts, factor):
    owner, partner = [(jnp.arange(values.shape[dim]) // (values.shape[dim] // parts)).reshape([-1 if axis == dim else 1 for axis in range(values.ndim)]) for dim in (source, target)]
    chosen = jax.random.permutation(key, parts)[partner]
    strong = (owner == chosen) | (owner == (partner + parts // 2) % parts)
    return jnp.where(strong, factor * values, values)


def block_scale(stream_key, shape, split, least, top_value):
    loudness, own = 1.0, jax.random.fold_in(stream_key, 6)
    for dim, parts in split:
        draws = jnp.exp(jax.random.uniform(jax.random.fold_in(own, dim), (parts,), jnp.float32, least / len(split), top_value / len(split)))
        loudness = loudness * jnp.repeat(draws, shape[dim] // parts).reshape([-1 if axis == dim else 1 for axis in range(len(shape))])
    return loudness


def profile(count, total, most, skew):
    loads = [(1 << 20) // math.isqrt(grade ** skew) + 1 for grade in range(2, count + 1)]
    spare, counts = total - most - (count - 1), [1] * (count - 1)
    while spare > 0:
        free = [i for i in range(count - 1) if counts[i] < most]
        whole, budget = sum([loads[i] for i in free]), spare
        for i in free:
            more = min(most - counts[i], max(1, budget * loads[i] // whole), spare)
            counts[i] = counts[i] + more
            spare = spare - more
    return np.array([most] + counts)


def ragged(own_key, count, total, reach, slope):
    if count == 2:
        one = jax.random.randint(own_key, (), max(1, total - reach), min(reach, total - 1) + 1)
        return jnp.stack([one, total - one])
    sizes = jnp.asarray(profile(count, total, reach, slope), jnp.int32)
    couples = (count - 1) // 2
    source_of, taker = sizes[1:1 + 2 * couples:2], sizes[2:2 + 2 * couples:2]
    slack = jnp.minimum(source_of - 1, reach - taker)
    passed = jax.random.randint(jax.random.fold_in(own_key, 1), (couples,), 0, 1 << 20) % (slack + 1)
    sizes = sizes.at[1:1 + 2 * couples:2].set(source_of - passed).at[2:2 + 2 * couples:2].set(taker + passed)
    return sizes[jax.random.permutation(jax.random.fold_in(own_key, 2), count)]


def normal_values(key, shape, scale, limit, pieces=(), held_as=jnp.bfloat16):
    gain = block_scale(key, shape, pieces, -0.22, 0.18) if pieces else 1.0
    array = jax.random.normal(key, shape, jnp.float32) * scale * gain
    return jnp.minimum(jnp.maximum(array, -limit), limit).astype(held_as)


def gaussian_with(own_key, extent, deviation, most, cuts, heavy, held_as=jnp.bfloat16):
    array = deviation * jax.random.normal(own_key, extent, jnp.float32)
    if cuts:
        array = array * block_scale(own_key, extent, cuts, -0.22, 0.18)
    return jnp.clip(strengthened(array, jax.random.fold_in(own_key, 3), *heavy), -most, most).astype(held_as)


def setup_inputs(seed: int = 0, part: int = 0) -> dict:
    arg_keys = jax.random.split(jax.random.key(seed), 9)
    part_keys = jax.random.split(jax.random.fold_in(arg_keys[8], part), 9)
    queries = draw_queries(jax.random.fold_in(jax.random.fold_in(arg_keys[8], part), 71), part)
    keys = draw_keys(jax.random.fold_in(jax.random.fold_in(arg_keys[8], part), 71), part)
    values = normal_values(part_keys[2], (CLIP_TOKENS, KEY_VALUE_HEADS * HEAD_WIDTH), 3.0, 18.0, ((0, 8), (1, 2)))
    half_order = draw_half_order(jax.random.fold_in(jax.random.fold_in(arg_keys[8], part), 71), part)
    frame_lengths = ragged(part_keys[4], FRAMES, CLIP_TOKENS, FRAME_MOST, 2).astype(jnp.int32)
    out_proj = gaussian_with(arg_keys[5], (QUERY_HEAD_COUNT * HEAD_WIDTH, OUT_WIDTH), (QUERY_HEAD_COUNT * HEAD_WIDTH) ** -0.5, 0.09375, ((0, 2), (1, 8)), (0, 1, 8, 2.0))
    residual_in = draw_residual_in(jax.random.fold_in(jax.random.fold_in(arg_keys[8], part), 71), part)
    norm_gain = jnp.clip(1.0 + 0.1 * jax.random.normal(arg_keys[7], (OUT_WIDTH,), jnp.float32), 0.5, 1.5)
    return dict(queries=queries, keys=keys, values=values, half_order=half_order, frame_lengths=frame_lengths, out_proj=out_proj, residual_in=residual_in, norm_gain=norm_gain)


def positions_of(half_order):
    row_ids = jnp.arange(CLIP_TOKENS, dtype=jnp.int32)
    return (half_order[row_ids // HALF] * HALF + row_ids % HALF).astype(jnp.int32)

def frame_limits(position, frame_lengths):
    frame_ends = jnp.cumsum(frame_lengths).astype(jnp.int32)
    frame_starts = frame_ends - frame_lengths
    chosen = jnp.where(frame_starts[None, :] <= position[:, None], frame_lengths[None, :], 0)
    return lax.optimization_barrier(jnp.sum(chosen, axis=1)).astype(jnp.int32)

def reference(queries, keys, values, half_order, frame_lengths, out_proj, residual_in, norm_gain):
    group_width = QUERY_HEAD_COUNT // KEY_VALUE_HEADS
    position = positions_of(half_order)
    frame_end = frame_limits(position, frame_lengths)
    query_head_rows = queries.reshape(CLIP_TOKENS, KEY_VALUE_HEADS, group_width, HEAD_WIDTH)
    key_head_rows = keys.reshape(CLIP_TOKENS, KEY_VALUE_HEADS, HEAD_WIDTH)
    value_head_rows = values.reshape(CLIP_TOKENS, KEY_VALUE_HEADS, HEAD_WIDTH)
    block_rows = min(512, CLIP_TOKENS)
    block_count = CLIP_TOKENS // block_rows

    def single_head(kv_head):
        key_one = key_head_rows[:, kv_head].astype(jnp.float32)
        value_one = value_head_rows[:, kv_head].astype(jnp.float32)
        query_one = query_head_rows[:, kv_head]

        def one_block(block_id):
            query_block = lax.dynamic_slice_in_dim(query_one, block_id * block_rows, block_rows, 0).astype(jnp.float32)
            limit_block = lax.dynamic_slice_in_dim(frame_end, block_id * block_rows, block_rows, 0)
            scores = jnp.einsum('qgd,kd->gqk', query_block, key_one) * HEAD_WIDTH ** (-0.5)
            visible = position[None, :] < limit_block[:, None]
            scores = jnp.where(visible[None], scores, -1e+30)
            row_max = lax.optimization_barrier(jnp.max(scores, axis=-1, keepdims=True))
            weights = jnp.where(visible[None], jnp.exp(scores - row_max), 0.0)
            total = lax.optimization_barrier(jnp.sum(weights, axis=-1))
            rounded = weights.astype(jnp.bfloat16).astype(jnp.float32)
            summed = jnp.einsum('gqk,kd->qgd', rounded, value_one)
            return (summed / jnp.transpose(total)[:, :, None]).astype(jnp.bfloat16)
        blocks = lax.map(one_block, jnp.arange(block_count, dtype=jnp.int32))
        return blocks.reshape(CLIP_TOKENS, group_width, HEAD_WIDTH)
    each_head_rows = lax.map(single_head, jnp.arange(KEY_VALUE_HEADS, dtype=jnp.int32))
    attended = jnp.transpose(each_head_rows, (1, 0, 2, 3)).reshape(CLIP_TOKENS, QUERY_HEAD_COUNT * HEAD_WIDTH)
    projected = jnp.dot(attended, out_proj, preferred_element_type=jnp.float32)
    hidden_state = (residual_in.astype(jnp.float32) + projected).astype(jnp.bfloat16)
    widened = hidden_state.astype(jnp.float32)
    energy = lax.optimization_barrier(jnp.sum(widened * widened, axis=-1)) / OUT_WIDTH
    normed = (widened * lax.rsqrt(energy + 1e-06)[:, None] * norm_gain.astype(jnp.float32)[None, :]).astype(jnp.bfloat16)
    return (attended, hidden_state, normed)
```

```python
import functools
import math

import jax
import jax.numpy as jnp
from jax import lax
from jax.experimental import pallas as pl
from jax.experimental.pallas import tpu as pltpu
from jax.sharding import PartitionSpec as P

HEAD_WIDTH = 128
MESH = pl.DeviceIdType.MESH


def loop(low, high, body):
    def step(i, carry):
        body(i)
        return carry

    lax.fori_loop(low, high, step, 0)


def kernel(dims, order_ref, frames_ref, q_hbm, k_hbm, v_hbm, proj_hbm, res_hbm, gain_hbm,
           att_out, hidden_out, normed_out,
           kvbuf, attbuf, wall, wext, q_ref, res_ref, gain_ref, bias, pbuf, xbuf, obuf, mbuf, retbuf, ebuf,
           in_sem, kv_in, kv_send, kv_recv, at_send, at_recv, x_send, x_recv, ret_send, ret_recv, m_recv,
           w_send, w_recv, wf_send, en_send, en_recv):
    S, C, H, G, Y, Q, NJ, hub, near = dims
    n = S * C
    blocks = n // H
    rows = q_ref.shape[0]
    width = q_ref.shape[1] // G
    deep, thin = wall.shape[1], wall.shape[2]
    total = n * rows
    part_rows = wext.shape[1] // Y
    piece_rows = part_rows // NJ
    pieces = Q * NJ
    steps = width // HEAD_WIDTH
    pack = 2 if steps % 2 == 0 else 1
    steps = steps // pack
    span = pack * HEAD_WIDTH
    pace, lead = min(3, steps), min(1, steps - 1)
    side_lag = min(2, G - 1)
    y, z = lax.axis_index("groups"), lax.axis_index("seq")
    c, h = lax.axis_index("sub"), lax.axis_index("heads")
    own = z * C + c
    inner = (z >= 1) & (z <= S - 2) if hub else (z >= 0)
    outer = jnp.logical_not(inner)
    is_hub = (z == 1) | (z == S - 2)
    edge = jnp.where(z < S // 2, 0, S - 1)
    hub_of_edge = jnp.where(z < S // 2, 1, S - 2)
    inward = jnp.where(z < S // 2, 1, -1)

    def reach(g):
        if not hub:
            return 0, S - 1
        return jnp.where(g < near, 0, 1), jnp.where(g < near, S - 1, S - 2)

    barrier = pltpu.get_barrier_semaphore()

    def greet(t):
        other = lax.rem(own * H + h + t, n * H)
        place = other // H
        pl.semaphore_signal(
            barrier, inc=1,
            device_id={"seq": place // C, "sub": place % C, "heads": other % H},
            device_id_type=MESH,
        )

    loop(1, n * H, greet)
    greeted = n * H - 1
    if hub:
        for k in range(1, Y):
            pl.semaphore_signal(barrier, inc=1, device_id={"groups": (y + k) % Y}, device_id_type=MESH)
        greeted += Y - 1

    kv_copies = []
    for g in range(G):
        part = slice(g * HEAD_WIDTH, (g + 1) * HEAD_WIDTH)
        kv_copies.append(pltpu.make_async_copy(k_hbm.at[:, part], kvbuf.at[own, g, 0], kv_in.at[g, 0]))
        kv_copies.append(pltpu.make_async_copy(v_hbm.at[:, part], kvbuf.at[own, g, 1], kv_in.at[g, 1]))
    for copy in kv_copies:
        copy.start()
    q_copy = pltpu.make_async_copy(q_hbm, q_ref, in_sem.at[0])
    q_copy.start()
    res_copy = pltpu.make_async_copy(res_hbm, res_ref, in_sem.at[1])
    res_copy.start()
    gain_copy = pltpu.make_async_copy(gain_hbm, gain_ref, in_sem.at[2])
    gain_copy.start()

    def own_weights(q, depth):
        return pltpu.make_async_copy(
            proj_hbm.at[:depth, q * thin:(q + 1) * thin], wall.at[q, :depth, :], in_sem.at[3 + q]
        )

    def each_own_weights(act):
        @pl.when(inner)
        def _():
            for q in range(Q):
                act(own_weights(q, deep))

        if hub and near:
            @pl.when(outer)
            def _():
                for q in range(Q):
                    act(own_weights(q, near * width))

    each_own_weights(lambda copy: copy.start())
    for copy in kv_copies:
        copy.wait()
    with jax.named_scope("barrier"):
        pl.semaphore_wait(barrier, greeted)

    def hop(buf, send, recv, side, zs, cs, g, cut=None):
        target = ({"seq": jnp.minimum(z + 1, S - 1)}, {"seq": jnp.maximum(z - 1, 0)}, {"sub": (c + 1) % C})[side]
        index = zs * C + cs
        block = buf.at[index, g] if cut is None else buf.at[index, g, :, cut]
        return pltpu.make_async_remote_copy(
            src_ref=block,
            dst_ref=block,
            send_sem=send.at[side, zs, g],
            recv_sem=recv.at[index, g],
            device_id=target,
            device_id_type=MESH,
        )

    def launch(buf, send, recv, g, lo, hi, cut=None):
        @pl.when(z + 1 <= hi)
        def _():
            hop(buf, send, recv, 0, z, c, g, cut).start()

        @pl.when(z - 1 >= lo)
        def _():
            hop(buf, send, recv, 1, z, c, g, cut).start()

        if C > 1:
            @pl.when((z >= lo) & (z <= hi))
            def _():
                hop(buf, send, recv, 2, z, c, g, cut).start()

    def relay_right(buf, send, recv, d, g, lo, hi):
        @pl.when((z - d >= 0) & (z >= lo) & (z <= hi))
        def _():
            hop(buf, send, recv, 0, z - d, c, g).wait_recv()

            @pl.when(z + 1 <= hi)
            def _():
                hop(buf, send, recv, 0, z - d, c, g).start()

            if C > 1:
                hop(buf, send, recv, 2, z - d, c, g).start()

    def relay_left(buf, send, recv, d, g, lo, hi):
        @pl.when((z + d < S) & (z >= lo) & (z <= hi))
        def _():
            hop(buf, send, recv, 1, z + d, c, g).wait_recv()

            @pl.when(z - 1 >= lo)
            def _():
                hop(buf, send, recv, 1, z + d, c, g).start()

            if C > 1:
                hop(buf, send, recv, 2, z + d, c, g).start()

    def from_partner(buf, send, recv, zs, g):
        if C > 1:
            hop(buf, send, recv, 2, zs, (c + 1) % C, g).wait_recv()

    def drain(buf, send, recv, zs, g, lo, hi):
        @pl.when((zs <= z) & (z + 1 <= hi))
        def _():
            hop(buf, send, recv, 0, zs, c, g).wait_send()

        @pl.when((zs >= z) & (z - 1 >= lo))
        def _():
            hop(buf, send, recv, 1, zs, c, g).wait_send()

        if C > 1:
            @pl.when((z >= lo) & (z <= hi))
            def _():
                hop(buf, send, recv, 2, zs, c, g).wait_send()

    def w_block(i, side):
        q, j = i // NJ, i % NJ
        return q, side * part_rows + j * piece_rows

    def w_out(i):
        q, at = w_block(i, y)
        return pltpu.make_async_remote_copy(
            src_ref=proj_hbm.at[
                pl.ds(pl.multiple_of(near * width + at, piece_rows), piece_rows),
                pl.ds(pl.multiple_of(q * thin, thin), thin),
            ],
            dst_ref=wext.at[q, pl.ds(pl.multiple_of(at, piece_rows), piece_rows), :],
            send_sem=w_send.at[i], recv_sem=w_recv.at[y, i],
            device_id={"seq": hub_of_edge}, device_id_type=MESH,
        )

    def w_pass(i, k, side):
        q, at = w_block(i, side)
        block = wext.at[q, pl.ds(pl.multiple_of(at, piece_rows), piece_rows), :]
        return pltpu.make_async_remote_copy(
            src_ref=block, dst_ref=block,
            send_sem=wf_send.at[k - 1, i], recv_sem=w_recv.at[side, i],
            device_id={"groups": (y + k) % Y}, device_id_type=MESH,
        )

    def w_relay(i):
        with jax.named_scope("wwait"):
            w_pass(i, 1, y).wait_recv()
        for k in range(1, Y):
            w_pass(i, k, y).start()

    def wave(s):
        @pl.when((s + 2 < G) & (inner if hub else True))
        def _():
            launch(kvbuf, kv_send, kv_recv, jnp.minimum(s + 2, G - 1), 0, S - 1)

        def one(d):
            g = s + 1 - d

            @pl.when((g >= 0) & (g < G))
            def _():
                at = jnp.clip(g, 0, G - 1)
                relay_right(kvbuf, kv_send, kv_recv, d, at, 0, S - 1)
                relay_left(kvbuf, kv_send, kv_recv, d, at, 0, S - 1)

        with jax.named_scope("wave"):
            loop(1, S, one)

    def kv_partner(g):
        with jax.named_scope("kvpartner"):
            loop(0, S, lambda s: from_partner(kvbuf, kv_send, kv_recv, s, g))

    loop(0, min(2, G), lambda g: launch(kvbuf, kv_send, kv_recv, g, 0, S - 1))
    if hub:
        @pl.when(outer)
        def _():
            loop(min(2, G), G, lambda g: launch(kvbuf, kv_send, kv_recv, g, 0, S - 1))
            loop(0, pieces, lambda i: w_out(i).start())

    half_rows = total // order_ref.shape[0]
    per_device = rows // half_rows
    lane = lax.broadcasted_iota(jnp.int32, (1, total), 1)
    key_pos = jnp.zeros((1, total), jnp.int32)
    for t in range(order_ref.shape[0]):
        inside = (lane >= t * half_rows) & (lane < (t + 1) * half_rows)
        key_pos = jnp.where(inside, lane + (order_ref[t] - t) * half_rows, key_pos)
    line = lax.broadcasted_iota(jnp.int32, (rows, 1), 0)
    row_pos = jnp.zeros((rows, 1), jnp.int32)
    for t in range(per_device):
        inside = (line >= t * half_rows) & (line < (t + 1) * half_rows)
        row_pos = jnp.where(inside, line + (order_ref[own * per_device + t] - t) * half_rows, row_pos)
    limit = jnp.zeros((rows, 1), jnp.int32)
    first = jnp.int32(0)
    for f in range(frames_ref.shape[0]):
        limit = limit + jnp.where(first <= row_pos, frames_ref[f], 0)
        first = first + frames_ref[f]
    bias[...] = jnp.where(key_pos < limit, 0.0, -1e30)

    factor = HEAD_WIDTH ** (-0.5) * math.log2(math.e)

    def attention(g):
        kv_partner(g)
        key = kvbuf[:, g, 0].reshape(total, HEAD_WIDTH)
        value = kvbuf[:, g, 1].reshape(total, HEAD_WIDTH)

        def few_heads(b):
            at = pl.multiple_of(g * width + b * span, span)
            q = q_ref[:, pl.ds(at, span)]
            q = jnp.concatenate(
                [q[:, k * HEAD_WIDTH:(k + 1) * HEAD_WIDTH] for k in range(pack)], axis=0
            )
            s = lax.dot_general(q, key, (((1,), (1,)), ((), ())), preferred_element_type=jnp.float32)
            s = (s.reshape(pack, rows, total) + bias[...][None]).reshape(pack * rows, total)
            top = jnp.max(s, axis=-1, keepdims=True)
            w = jnp.exp2((s - top) * factor)
            amount = jnp.sum(w, axis=-1, keepdims=True)
            o = jnp.dot(w.astype(jnp.bfloat16), value, preferred_element_type=jnp.float32)
            o = (o / amount).astype(jnp.bfloat16)
            o = jnp.concatenate([o[k * rows:(k + 1) * rows] for k in range(pack)], axis=1)
            att_out[:, pl.ds(at, span)] = o
            cut = pl.ds(pl.multiple_of(b * span, span), span)
            attbuf[own, g, :, cut] = o
            launch(attbuf, at_send, at_recv, g, *reach(g), cut)

            turn = g * steps + b - lead

            @pl.when((turn >= 0) & (turn % pace == 0) & (turn // pace < G - 1))
            def _():
                wave(S - 1 + turn // pace)

        loop(0, steps, few_heads)

    def x_copy(t, u):
        return pltpu.make_async_remote_copy(
            src_ref=pbuf.at[u, t],
            dst_ref=xbuf.at[u, t // H, h],
            send_sem=x_send.at[u, t],
            recv_sem=x_recv.at[u, t // H, h],
            device_id={"heads": t % H},
            device_id_type=MESH,
        )

    def multiply(zb, u, weights, g0, g1):
        summed = jnp.zeros((C * rows, thin), jnp.float32)
        for g in range(g0, g1):
            summed = summed + jnp.dot(
                attbuf[pl.ds(zb * C, C), g].reshape(C * rows, width),
                weights[u % Q, (g - g0) * width:(g - g0 + 1) * width, :],
                preferred_element_type=jnp.float32,
            )
        summed = summed.astype(jnp.bfloat16)
        for k in range(C):
            t = zb * C + k
            mine = t % H == h

            @pl.when(mine)
            def _():
                xbuf[u, t // H, h] = summed[k * rows:(k + 1) * rows]

            @pl.when(jnp.logical_not(mine))
            def _():
                pbuf[u, t] = summed[k * rows:(k + 1) * rows]
                x_copy(t, u).start()

    def place_of(u):
        block = jnp.where(u < Q, own, edge * C + c)
        return block // blocks, block % blocks, u % Q

    def result_copy(t, u):
        home, slot, q = place_of(u)
        return pltpu.make_async_remote_copy(
            src_ref=obuf.at[u, t // H],
            dst_ref=retbuf.at[slot, q],
            send_sem=ret_send.at[u, t // H],
            recv_sem=ret_recv.at[slot, q],
            device_id={"seq": t // C, "sub": t % C, "heads": home},
            device_id_type=MESH,
        )

    def merge_copy(t, u):
        return pltpu.make_async_remote_copy(
            src_ref=obuf.at[u, t // H],
            dst_ref=mbuf.at[u % Q, t // H],
            send_sem=ret_send.at[u, t // H],
            recv_sem=m_recv.at[u % Q, t // H],
            device_id={"seq": hub_of_edge},
            device_id_type=MESH,
        )

    def reduce(zb, u):
        home, slot, q = place_of(u)
        for k in range(C):
            t = zb * C + k

            @pl.when(t % H == h)
            def _():
                value = jnp.zeros((rows, thin), jnp.float32)
                for other in range(H):
                    @pl.when(other != h)
                    def _():
                        pltpu.make_async_remote_copy(
                            src_ref=pbuf.at[u, t], dst_ref=xbuf.at[u, t // H, other],
                            send_sem=x_send.at[u, t], recv_sem=x_recv.at[u, t // H, other],
                            device_id={"heads": (h + 1) % H}, device_id_type=MESH,
                        ).wait_recv()
                    value = value + xbuf[u, t // H, other].astype(jnp.float32)
                obuf[u, t // H] = value.astype(jnp.bfloat16)
                if hub and near:
                    @pl.when(u >= Q)
                    def _():
                        merge_copy(t, u).wait_recv()
                        obuf[u, t // H] = (value + mbuf[q, t // H].astype(jnp.float32)).astype(jnp.bfloat16)

                    @pl.when(outer)
                    def _():
                        merge_copy(t, u).start()
                here = (t == own) & (home == h)

                @pl.when(inner & here)
                def _():
                    retbuf[slot, q] = obuf[u, t // H]

                @pl.when(inner & jnp.logical_not(here))
                def _():
                    result_copy(t, u).start()

    def multiply_all(zb):
        @pl.when(inner)
        def _():
            with jax.named_scope("arrive"):
                loop(0, G, lambda g: from_partner(attbuf, at_send, at_recv, zb, g))
            with jax.named_scope("mult"):
                loop(0, Q, lambda u: multiply(zb, u, wall, 0, G))

        if hub and near:
            @pl.when(outer)
            def _():
                with jax.named_scope("arrive"):
                    loop(0, near, lambda g: from_partner(attbuf, at_send, at_recv, zb, g))
                with jax.named_scope("multend"):
                    loop(0, Q, lambda u: multiply(zb, u, wall, 0, near))

    def multiply_extra(zb):
        @pl.when(is_hub)
        def _():
            with jax.named_scope("extra"):
                loop(Q, 2 * Q, lambda u: multiply(zb, u, wext, near, G))

    def reduce_extra(zb):
        @pl.when(is_hub)
        def _():
            with jax.named_scope("reduceextra"):
                loop(Q, 2 * Q, lambda u: reduce(zb, u))

    def reduce_all(zb):
        with jax.named_scope("reduce"):
            @pl.when((inner | outer) if near else inner)
            def _():
                loop(0, Q, lambda u: reduce(zb, u))

    def by_slot(k, act, self_slot):
        def pick(which):
            since = jnp.where(which == 2, k - side_lag, k)
            d = jnp.where(which == 0, 0, since // G + 1)
            zb = z + jnp.where(which == 2, -inward, inward) * d
            due = jnp.where(which == 0, k == self_slot, (since >= 0) & (since % G == G - 1))

            @pl.when(due & (zb >= 0) & (zb < S))
            def _():
                act(jnp.clip(zb, 0, S - 1))

        loop(0, 3, pick)

    def relay_slot(k, rightward):
        d, g = k // G + 1, k % G
        move = relay_right if rightward else relay_left
        move(attbuf, at_send, at_recv, d, g, *reach(g))

    loop(0, S - 1, wave)
    q_copy.wait()

    def head_step(g):
        with jax.named_scope("attention"):
            attention(g)
        if hub:
            for k in range(2):
                @pl.when(is_hub & (g > 0) & ((g - 1) * 2 + k < pieces))
                def _():
                    w_relay((g - 1) * 2 + k)

    loop(0, G, head_step)
    each_own_weights(lambda copy: copy.wait())

    def slot_step(k):
        if hub:
            @pl.when(is_hub & (k == min(1, side_lag)))
            def _():
                loop(min(pieces, 2 * (G - 1)), pieces, w_relay)

        with jax.named_scope("arelay"):
            for rightward in (False, True):
                inner_side = (inward < 0) if rightward else (inward > 0)
                at = jnp.where(inner_side, k, k - side_lag)

                @pl.when(at >= 0)
                def _():
                    relay_slot(jnp.maximum(at, 0), rightward)

        if hub:
            @pl.when(is_hub & (k == side_lag))
            def _():
                with jax.named_scope("wother"):
                    for t in range(1, Y):
                        loop(0, pieces, lambda i: w_pass(i, 1, (y + t) % Y).wait_recv())

        by_slot(k, multiply_all, 0)
        if hub:
            by_slot(k, multiply_extra, side_lag)

        @pl.when(k > 0)
        def _():
            by_slot(k - 1, reduce_all, 0)

    slots = (S - 1) * G + side_lag
    loop(0, slots, slot_step)
    by_slot(slots - 1, reduce_all, 0)
    if hub:
        loop(0, slots, lambda k: by_slot(k, reduce_extra, side_lag))

    res_copy.wait()
    squares = jnp.zeros((rows, 1), jnp.float32)
    for b in range(blocks):
        block = h * blocks + b
        source = block // C
        if hub:
            source = jnp.clip(source, 1, S - 2)
        made_here = (source == z) & (block % C == c) & (own % H == h)
        for q in range(Q):
            @pl.when(jnp.logical_not(made_here))
            def _():
                with jax.named_scope(f"final{b}_{q}"):
                    pltpu.make_async_remote_copy(
                        src_ref=obuf.at[0, 0], dst_ref=retbuf.at[b, q],
                        send_sem=ret_send.at[0, 0], recv_sem=ret_recv.at[b, q],
                        device_id={"heads": (h + 1) % H}, device_id_type=MESH,
                    ).wait_recv()
            where = slice((b * Q + q) * thin, (b * Q + q + 1) * thin)
            hidden = (res_ref[:, where].astype(jnp.float32) + retbuf[b, q].astype(jnp.float32)).astype(jnp.bfloat16)
            hidden_out[:, where] = hidden
            wide = hidden.astype(jnp.float32)
            squares = squares + jnp.sum(wide * wide, axis=-1, keepdims=True)

    ebuf[h] = jnp.broadcast_to(squares, (rows, 128))

    def share(k, side):
        other = (h + k) % H if side == 0 else (h + H - k) % H
        return pltpu.make_async_remote_copy(
            src_ref=ebuf.at[h], dst_ref=ebuf.at[h if side == 0 else other],
            send_sem=en_send.at[k], recv_sem=en_recv.at[h if side == 0 else other],
            device_id={"heads": (h + k) % H}, device_id_type=MESH,
        )

    for k in range(1, H):
        share(k, 0).start()
    with jax.named_scope("energy"):
        for k in range(1, H):
            share(k, 1).wait_recv()
    energy = ebuf[0]
    for k in range(1, H):
        energy = energy + ebuf[k]
    inverse = lax.rsqrt(energy[:, 0:1] / (H * res_ref.shape[1]) + 1e-06)
    gain_copy.wait()
    for b in range(blocks):
        where = slice(b * Q * thin, (b + 1) * Q * thin)
        normed_out[:, where] = (
            hidden_out[:, where].astype(jnp.float32) * inverse * gain_ref[:, where]
        ).astype(jnp.bfloat16)

    for k in range(1, H):
        share(k, 0).wait_send()

    def finish(i):
        zs, g = i // G, i % G
        drain(kvbuf, kv_send, kv_recv, zs, g, 0, S - 1)
        drain(attbuf, at_send, at_recv, zs, g, *reach(g))

    with jax.named_scope("drain"):
        loop(0, S * G, finish)

    def finish_results(u):
        home, slot, q = place_of(u)

        def finish_one(t):
            @pl.when(t % H != h)
            def _():
                x_copy(t, u).wait_send()

            @pl.when(inner & (t % H == h) & jnp.logical_not((t == own) & (home == h)))
            def _():
                result_copy(t, u).wait_send()

            if hub and near:
                @pl.when(outer & (t % H == h))
                def _():
                    merge_copy(t, u).wait_send()

        @pl.when(((u < Q) & ((inner | outer) if near else inner)) | ((u >= Q) & is_hub))
        def _():
            loop(0, n, finish_one)

    loop(0, Q * (2 if hub else 1), finish_results)

    if hub:
        @pl.when(outer)
        def _():
            loop(0, pieces, lambda i: w_out(i).wait_send())

        @pl.when(is_hub)
        def _():
            for k in range(1, Y):
                loop(0, pieces, lambda i: w_pass(i, k, y).wait_send())


def shards(dims, queries, keys, values, half_order, frame_lengths, out_proj, residual_in, norm_gain):
    S, C, H, Y = dims
    n = S * C
    rows = queries.shape[0]
    G = keys.shape[1] // HEAD_WIDTH
    width = queries.shape[1] // G
    deep, cols = out_proj.shape
    hub = S >= 4
    Q = 2 if cols % 512 == 0 else 1
    NJ = 4
    near = G // 2
    thin = cols // Q
    U = Q * (2 if hub else 1)
    hbm = pl.BlockSpec(memory_space=pltpu.HBM)
    vmem = pl.BlockSpec(memory_space=pltpu.VMEM)
    smem = pl.BlockSpec(memory_space=pltpu.SMEM)
    dma = pltpu.SemaphoreType.DMA
    bf16, f32 = jnp.bfloat16, jnp.float32
    return pl.pallas_call(
        functools.partial(kernel, (S, C, H, G, Y, Q, NJ, hub, near)),
        out_shape=(
            jax.ShapeDtypeStruct(queries.shape, bf16),
            jax.ShapeDtypeStruct(residual_in.shape, bf16),
            jax.ShapeDtypeStruct(residual_in.shape, bf16),
        ),
        in_specs=[smem, smem, hbm, hbm, hbm, hbm, hbm, hbm],
        out_specs=(vmem, vmem, vmem),
        scratch_shapes=[
            pltpu.VMEM((n, G, 2, rows, HEAD_WIDTH), bf16),
            pltpu.VMEM((n, G, rows, width), bf16),
            pltpu.VMEM((Q, deep, thin), bf16),
            pltpu.VMEM((Q, (G - near) * width, thin), bf16),
            pltpu.VMEM(queries.shape, bf16),
            pltpu.VMEM(residual_in.shape, bf16),
            pltpu.VMEM((1, norm_gain.shape[0]), f32),
            pltpu.VMEM((rows, n * rows), f32),
            pltpu.VMEM((U, n, rows, thin), bf16),
            pltpu.VMEM((U, n // H, H, rows, thin), bf16),
            pltpu.VMEM((U, n // H, rows, thin), bf16),
            pltpu.VMEM((Q, n // H, rows, thin), bf16),
            pltpu.VMEM((n // H, Q, rows, thin), bf16),
            pltpu.VMEM((H, rows, 128), f32),
            dma((3 + Q,)),
            dma((G, 2)),
            dma((3, S, G)),
            dma((n, G)),
            dma((3, S, G)),
            dma((n, G)),
            dma((U, n)),
            dma((U, n // H, H)),
            dma((U, n // H)),
            dma((n // H, Q)),
            dma((Q, n // H)),
            dma((Q * NJ,)),
            dma((Y, Q * NJ)),
            dma((max(Y - 1, 1), Q * NJ)),
            dma((H,)),
            dma((H,)),
        ],
        compiler_params=pltpu.CompilerParams(
            collective_id=0, has_side_effects=True, vmem_limit_bytes=51 * 1024 * 1024
        ),
    )(half_order, frame_lengths, queries, keys, values, out_proj, residual_in, norm_gain[None, :])


def solution(mesh):
    dims = (mesh.shape["seq"], mesh.shape["sub"], mesh.shape["heads"], mesh.shape["groups"])
    token = P(("groups", "seq", "sub"), "heads")
    in_specs = (
        token, token, token, P("groups"), P("groups"),
        P("heads", ("seq", "sub")), token, P("heads"),
    )
    return jax.shard_map(
        functools.partial(shards, dims), mesh=mesh, in_specs=in_specs,
        out_specs=(token, token, token), check_vma=False,
    )
```

```python
import functools
import math

import jax
import jax.numpy as jnp
from jax import lax
from jax.experimental import pallas as pl
from jax.experimental.pallas import tpu as pltpu
from jax.sharding import PartitionSpec as P

HEAD_WIDTH = 128
MESH = pl.DeviceIdType.MESH


def loop(low, high, body):
    def step(i, carry):
        body(i)
        return carry

    lax.fori_loop(low, high, step, 0)


def kernel(dims, order_hbm, frames_hbm, q_hbm, k_hbm, v_hbm, proj_hbm, res_hbm, gain_hbm,
           att_hbm, hidden_hbm, normed_hbm,
           order_ref, frames_ref, hidden_out, normed_out, acc, kvbuf, attbuf, wall, wext, q_ref, res_ref, gain_ref, bias, pbuf, xbuf, obuf, mbuf, retbuf, ebuf,
           in_sem, out_sem, kv_in, kv_send, kv_recv, at_send, at_recv, x_send, x_recv, ret_send, ret_recv, m_recv,
           w_send, w_recv, wf_send, en_send, en_recv):
    S, C, H, G, Y, Q, NJ, hub, near = dims
    n = S * C
    blocks = n // H
    rows = q_ref.shape[0]
    width = q_ref.shape[1] // G
    deep, thin = wall.shape[1], wall.shape[2]
    total = n * rows
    part_rows = wext.shape[1] // Y
    piece_rows = part_rows // NJ
    pieces = Q * NJ
    steps = width // HEAD_WIDTH
    pack = 2 if steps % 2 == 0 else 1
    steps = steps // pack
    span = pack * HEAD_WIDTH
    pace, lead = min(3, steps), min(1, steps - 1)
    R = 2 if steps % 2 == 0 else 1
    E = G * R
    cut_width = width // R
    side_lag = E // 2
    self_done = E // 2
    extra_slot = min(side_lag + 2, E - 1)
    y, z = lax.axis_index("groups"), lax.axis_index("seq")
    c, h = lax.axis_index("sub"), lax.axis_index("heads")
    own = z * C + c
    inner = (z >= 1) & (z <= S - 2) if hub else (z >= 0)
    outer = jnp.logical_not(inner)
    is_hub = (z == 1) | (z == S - 2)
    edge = jnp.where(z < S // 2, 0, S - 1)
    hub_of_edge = jnp.where(z < S // 2, 1, S - 2)
    inward = jnp.where(z < S // 2, 1, -1)

    def reach(g):
        if not hub:
            return 0, S - 1
        return jnp.where(g < near * R, 0, 1), jnp.where(g < near * R, S - 1, S - 2)

    kv_copies = []
    for g in range(G):
        part = slice(g * HEAD_WIDTH, (g + 1) * HEAD_WIDTH)
        kv_copies.append(pltpu.make_async_copy(k_hbm.at[:, part], kvbuf.at[own, g, 0], kv_in.at[g, 0]))
        kv_copies.append(pltpu.make_async_copy(v_hbm.at[:, part], kvbuf.at[own, g, 1], kv_in.at[g, 1]))
    for copy in kv_copies:
        copy.start()
    table_copies = [
        pltpu.make_async_copy(order_hbm, order_ref, in_sem.at[3]),
        pltpu.make_async_copy(frames_hbm, frames_ref, in_sem.at[4]),
    ]
    for copy in table_copies:
        copy.start()
    q_copy = pltpu.make_async_copy(q_hbm, q_ref, in_sem.at[0])
    q_copy.start()
    barrier = pltpu.get_barrier_semaphore()

    def greet(t):
        other = lax.rem(own * H + h + t, n * H)
        place = other // H
        pl.semaphore_signal(
            barrier, inc=1,
            device_id={"seq": place // C, "sub": place % C, "heads": other % H},
            device_id_type=MESH,
        )

    loop(1, n * H, greet)
    greeted = n * H - 1
    if hub:
        for k in range(1, Y):
            pl.semaphore_signal(barrier, inc=1, device_id={"groups": (y + k) % Y}, device_id_type=MESH)
        greeted += Y - 1

    res_copy = pltpu.make_async_copy(res_hbm, res_ref, in_sem.at[1])
    res_copy.start()
    gain_copy = pltpu.make_async_copy(gain_hbm, gain_ref, in_sem.at[2])
    gain_copy.start()

    def own_weights(q, depth):
        return pltpu.make_async_copy(
            proj_hbm.at[:depth, q * thin:(q + 1) * thin], wall.at[q, :depth, :], in_sem.at[5 + q]
        )

    def each_own_weights(act):
        @pl.when(inner)
        def _():
            for q in range(Q):
                act(own_weights(q, deep))

        if hub and near:
            @pl.when(outer)
            def _():
                for q in range(Q):
                    act(own_weights(q, near * width))

    each_own_weights(lambda copy: copy.start())
    with jax.named_scope("kvload"):
        for copy in kv_copies:
            copy.wait()
    with jax.named_scope("barrier"):
        pl.semaphore_wait(barrier, greeted)

    def hop(buf, send, recv, side, zs, cs, g, cut=None):
        target = ({"seq": jnp.minimum(z + 1, S - 1)}, {"seq": jnp.maximum(z - 1, 0)}, {"sub": (c + 1) % C})[side]
        index = zs * C + cs
        if buf is kvbuf:
            block = buf.at[index, g]
        else:
            if cut is None:
                cut = pl.ds(pl.multiple_of(g % R * cut_width, HEAD_WIDTH), cut_width)
            block = buf.at[index, g // R, :, cut]
        return pltpu.make_async_remote_copy(
            src_ref=block,
            dst_ref=block,
            send_sem=send.at[side, zs, g],
            recv_sem=recv.at[index, g],
            device_id=target,
            device_id_type=MESH,
        )

    def launch(buf, send, recv, g, lo, hi, cut=None, ways=None):
        inward_too, edgeward_too = ways or (True, True)

        @pl.when((z + 1 <= hi) & jnp.where(inward > 0, inward_too, edgeward_too))
        def _():
            hop(buf, send, recv, 0, z, c, g, cut).start()

        @pl.when((z - 1 >= lo) & jnp.where(inward < 0, inward_too, edgeward_too))
        def _():
            hop(buf, send, recv, 1, z, c, g, cut).start()

        if C > 1 and inward_too:
            @pl.when((z >= lo) & (z <= hi))
            def _():
                hop(buf, send, recv, 2, z, c, g, cut).start()

    def relay_right(buf, send, recv, d, g, lo, hi):
        @pl.when((z - d >= 0) & (z >= lo) & (z <= hi))
        def _():
            hop(buf, send, recv, 0, z - d, c, g).wait_recv()

            @pl.when(z + 1 <= hi)
            def _():
                hop(buf, send, recv, 0, z - d, c, g).start()

            if C > 1:
                hop(buf, send, recv, 2, z - d, c, g).start()

    def relay_left(buf, send, recv, d, g, lo, hi):
        @pl.when((z + d < S) & (z >= lo) & (z <= hi))
        def _():
            hop(buf, send, recv, 1, z + d, c, g).wait_recv()

            @pl.when(z - 1 >= lo)
            def _():
                hop(buf, send, recv, 1, z + d, c, g).start()

            if C > 1:
                hop(buf, send, recv, 2, z + d, c, g).start()

    def from_partner(buf, send, recv, zs, g):
        if C > 1:
            hop(buf, send, recv, 2, zs, (c + 1) % C, g).wait_recv()

    def drain(buf, send, recv, zs, g, lo, hi):
        @pl.when((zs <= z) & (z + 1 <= hi))
        def _():
            hop(buf, send, recv, 0, zs, c, g).wait_send()

        @pl.when((zs >= z) & (z - 1 >= lo))
        def _():
            hop(buf, send, recv, 1, zs, c, g).wait_send()

        if C > 1:
            @pl.when((z >= lo) & (z <= hi))
            def _():
                hop(buf, send, recv, 2, zs, c, g).wait_send()

    def w_block(i, side):
        q, j = i // NJ, i % NJ
        return q, side * part_rows + j * piece_rows

    def w_out(i):
        q, at = w_block(i, y)
        return pltpu.make_async_remote_copy(
            src_ref=proj_hbm.at[
                pl.ds(pl.multiple_of(near * width + at, piece_rows), piece_rows),
                pl.ds(pl.multiple_of(q * thin, thin), thin),
            ],
            dst_ref=wext.at[q, pl.ds(pl.multiple_of(at, piece_rows), piece_rows), :],
            send_sem=w_send.at[i], recv_sem=w_recv.at[y, i],
            device_id={"seq": hub_of_edge}, device_id_type=MESH,
        )

    def w_pass(i, k, side):
        q, at = w_block(i, side)
        block = wext.at[q, pl.ds(pl.multiple_of(at, piece_rows), piece_rows), :]
        return pltpu.make_async_remote_copy(
            src_ref=block, dst_ref=block,
            send_sem=wf_send.at[k - 1, i], recv_sem=w_recv.at[side, i],
            device_id={"groups": (y + k) % Y}, device_id_type=MESH,
        )

    def w_relay(i):
        with jax.named_scope("wwait"):
            w_pass(i, 1, y).wait_recv()
        for k in range(1, Y):
            w_pass(i, k, y).start()

    def wave(s):
        @pl.when((s + 2 < G) & (inner if hub else True))
        def _():
            launch(kvbuf, kv_send, kv_recv, jnp.minimum(s + 2, G - 1), 0, S - 1)

        def either(d, ahead):
            g = s + 1 - d + ahead

            @pl.when((g >= 0) & (g < G))
            def _():
                at = jnp.clip(g, 0, G - 1)

                @pl.when((inward > 0) == (ahead > 0))
                def _():
                    relay_right(kvbuf, kv_send, kv_recv, d, at, 0, S - 1)

                @pl.when((inward < 0) == (ahead > 0))
                def _():
                    relay_left(kvbuf, kv_send, kv_recv, d, at, 0, S - 1)

        def one(d):
            either(d, 1)
            either(d, 0)

        with jax.named_scope("wave"):
            loop(1, S, one)

    def kv_partner(g):
        with jax.named_scope("kvpartner"):
            loop(0, S, lambda s: from_partner(kvbuf, kv_send, kv_recv, s, g))

    loop(0, min(2, G), lambda g: launch(kvbuf, kv_send, kv_recv, g, 0, S - 1))
    if hub:
        @pl.when(outer)
        def _():
            loop(min(2, G), G, lambda g: launch(kvbuf, kv_send, kv_recv, g, 0, S - 1))
            loop(0, pieces, lambda i: w_out(i).start())

    for copy in table_copies:
        copy.wait()
    half_rows = total // order_ref.shape[0]
    per_device = rows // half_rows
    lane = lax.broadcasted_iota(jnp.int32, (1, total), 1)
    key_pos = jnp.zeros((1, total), jnp.int32)
    for t in range(order_ref.shape[0]):
        inside = (lane >= t * half_rows) & (lane < (t + 1) * half_rows)
        key_pos = jnp.where(inside, lane + (order_ref[t] - t) * half_rows, key_pos)
    line = lax.broadcasted_iota(jnp.int32, (rows, 1), 0)
    row_pos = jnp.zeros((rows, 1), jnp.int32)
    for t in range(per_device):
        inside = (line >= t * half_rows) & (line < (t + 1) * half_rows)
        row_pos = jnp.where(inside, line + (order_ref[own * per_device + t] - t) * half_rows, row_pos)
    limit = jnp.zeros((rows, 1), jnp.int32)
    first = jnp.int32(0)
    for f in range(frames_ref.shape[0]):
        limit = limit + jnp.where(first <= row_pos, frames_ref[f], 0)
        first = first + frames_ref[f]
    bias[...] = jnp.where(key_pos < limit, 0.0, -1e30)

    factor = HEAD_WIDTH ** (-0.5) * math.log2(math.e)

    def attention(g):
        kv_partner(g)
        key = kvbuf[:, g, 0].reshape(total, HEAD_WIDTH)
        value = kvbuf[:, g, 1].reshape(total, HEAD_WIDTH)

        def few_heads(b):
            at = pl.multiple_of(g * width + b * span, span)
            q = q_ref[:, pl.ds(at, span)]
            q = jnp.concatenate(
                [q[:, k * HEAD_WIDTH:(k + 1) * HEAD_WIDTH] for k in range(pack)], axis=0
            )
            s = lax.dot_general(q, key, (((1,), (1,)), ((), ())), preferred_element_type=jnp.float32)
            s = (s.reshape(pack, rows, total) + bias[...][None]).reshape(pack * rows, total)
            top = jnp.max(s, axis=-1, keepdims=True)
            w = jnp.exp2((s - top) * factor)
            amount = jnp.sum(w, axis=-1, keepdims=True)
            o = jnp.dot(w.astype(jnp.bfloat16), value, preferred_element_type=jnp.float32)
            o = (o / amount).astype(jnp.bfloat16)
            o = jnp.concatenate([o[k * rows:(k + 1) * rows] for k in range(pack)], axis=1)
            cut = pl.ds(pl.multiple_of(b * span, span), span)
            attbuf[own, g, :, cut] = o
            e = g * R + b * R // steps
            launch(attbuf, at_send, at_recv, e, *reach(e), cut, (True, False))

            turn = g * steps + b - lead

            @pl.when((turn >= 0) & (turn % pace == 0) & (turn // pace < G - 1))
            def _():
                wave(S - 1 + turn // pace)

        loop(0, steps, few_heads)

    def x_copy(t, u):
        return pltpu.make_async_remote_copy(
            src_ref=pbuf.at[u, t],
            dst_ref=xbuf.at[u, t // H, h],
            send_sem=x_send.at[u, t],
            recv_sem=x_recv.at[u, t // H, h],
            device_id={"heads": t % H},
            device_id_type=MESH,
        )

    def dots(summed, zb, u, weights, g0, g1, base):
        for g in range(g0, g1):
            summed = summed + jnp.dot(
                attbuf[pl.ds(zb * C, C), g].reshape(C * rows, width),
                weights[u % Q, (g - base) * width:(g - base + 1) * width, :],
                preferred_element_type=jnp.float32,
            )
        return summed

    def multiply_part(zb, u, weights, g0, g1, base):
        acc[u] = dots(jnp.zeros((C * rows, thin), jnp.float32), zb, u, weights, g0, g1, base)

    def multiply(zb, u, weights, g0, g1, base, more=False):
        start = acc[u] if more else jnp.zeros((C * rows, thin), jnp.float32)
        summed = dots(start, zb, u, weights, g0, g1, base)
        summed = summed.astype(jnp.bfloat16)
        for k in range(C):
            t = zb * C + k
            mine = t % H == h

            @pl.when(mine)
            def _():
                xbuf[u, t // H, h] = summed[k * rows:(k + 1) * rows]

            @pl.when(jnp.logical_not(mine))
            def _():
                pbuf[u, t] = summed[k * rows:(k + 1) * rows]
                x_copy(t, u).start()

    def place_of(u):
        block = jnp.where(u < Q, own, edge * C + c)
        return block // blocks, block % blocks, u % Q

    def result_copy(t, u):
        home, slot, q = place_of(u)
        return pltpu.make_async_remote_copy(
            src_ref=obuf.at[u, t // H],
            dst_ref=retbuf.at[slot, q],
            send_sem=ret_send.at[u, t // H],
            recv_sem=ret_recv.at[slot, q],
            device_id={"seq": t // C, "sub": t % C, "heads": home},
            device_id_type=MESH,
        )

    def merge_copy(t, u):
        return pltpu.make_async_remote_copy(
            src_ref=obuf.at[u, t // H],
            dst_ref=mbuf.at[u % Q, t // H],
            send_sem=ret_send.at[u, t // H],
            recv_sem=m_recv.at[u % Q, t // H],
            device_id={"seq": hub_of_edge},
            device_id_type=MESH,
        )

    def reduce(zb, u):
        home, slot, q = place_of(u)
        for k in range(C):
            t = zb * C + k

            @pl.when(t % H == h)
            def _():
                value = jnp.zeros((rows, thin), jnp.float32)
                for other in range(H):
                    @pl.when(other != h)
                    def _():
                        pltpu.make_async_remote_copy(
                            src_ref=pbuf.at[u, t], dst_ref=xbuf.at[u, t // H, other],
                            send_sem=x_send.at[u, t], recv_sem=x_recv.at[u, t // H, other],
                            device_id={"heads": (h + 1) % H}, device_id_type=MESH,
                        ).wait_recv()
                    value = value + xbuf[u, t // H, other].astype(jnp.float32)
                obuf[u, t // H] = value.astype(jnp.bfloat16)
                if hub and near:
                    @pl.when(u >= Q)
                    def _():
                        merge_copy(t, u).wait_recv()
                        obuf[u, t // H] = (value + mbuf[q, t // H].astype(jnp.float32)).astype(jnp.bfloat16)

                    @pl.when(outer)
                    def _():
                        merge_copy(t, u).start()
                here = (t == own) & (home == h)

                @pl.when(inner & here)
                def _():
                    retbuf[slot, q] = obuf[u, t // H]

                @pl.when(inner & jnp.logical_not(here))
                def _():
                    result_copy(t, u).start()

    def arrive(zb, e0, e1):
        with jax.named_scope("arrive"):
            loop(e0, e1, lambda e: from_partner(attbuf, at_send, at_recv, zb, e))

    def multiply_all(zb):
        @pl.when(inner)
        def _():
            arrive(zb, 0, E)
            with jax.named_scope("mult"):
                loop(0, Q, lambda u: multiply(zb, u, wall, 0, G, 0))

        if hub and near:
            @pl.when(outer)
            def _():
                arrive(zb, 0, near * R)
                with jax.named_scope("multend"):
                    loop(0, Q, lambda u: multiply(zb, u, wall, 0, near, 0))

    def multiply_extra(zb):
        @pl.when(is_hub)
        def _():
            with jax.named_scope("extra"):
                loop(Q, 2 * Q, lambda u: multiply(zb, u, wext, near, G, near))

    def multiply_most(zb):
        arrive(zb, 0, (G - 1) * R)
        with jax.named_scope("most"):
            loop(0, Q, lambda u: multiply_part(zb, u, wall, 0, G - 1, 0))
            loop(Q, 2 * Q, lambda u: multiply_part(zb, u, wext, near, G - 1, near))

    def multiply_last(zb):
        arrive(zb, (G - 1) * R, E)
        with jax.named_scope("last"):
            loop(0, Q, lambda u: multiply(zb, u, wall, G - 1, G, 0, True))
            loop(Q, 2 * Q, lambda u: multiply(zb, u, wext, G - 1, G, near, True))

    def reduce_extra(zb):
        @pl.when(is_hub)
        def _():
            with jax.named_scope("reduceextra"):
                loop(Q, 2 * Q, lambda u: reduce(zb, u))

    def reduce_all(zb):
        with jax.named_scope("reduce"):
            @pl.when((inner | outer) if near else inner)
            def _():
                loop(0, Q, lambda u: reduce(zb, u))

    def by_slot(k, act, self_slot):
        def pick(which):
            since = jnp.where(which == 2, k - side_lag, k)
            d = jnp.where(which == 0, 0, since // E + 1)
            zb = z + jnp.where(which == 2, -inward, inward) * d
            due = jnp.where(which == 0, k == self_slot, (since >= 0) & (since % E == E - 1))

            @pl.when(due & (zb >= 0) & (zb < S))
            def _():
                act(jnp.clip(zb, 0, S - 1))

        loop(0, 3, pick)

    def relay_slot(k, rightward):
        d, g = k // E + 1, k % E
        move = relay_right if rightward else relay_left
        move(attbuf, at_send, at_recv, d, g, *reach(g))

    @pl.when(inward > 0)
    def _():
        relay_right(kvbuf, kv_send, kv_recv, 1, 0, 0, S - 1)

    @pl.when(inward < 0)
    def _():
        relay_left(kvbuf, kv_send, kv_recv, 1, 0, 0, S - 1)

    loop(0, S - 1, wave)
    q_copy.wait()

    def att_copy(g):
        return pltpu.make_async_copy(
            attbuf.at[own, g], att_hbm.at[:, pl.ds(pl.multiple_of(g * width, width), width)], out_sem.at[2 + g]
        )

    def head_step(g):
        with jax.named_scope("attention"):
            attention(g)
        att_copy(g).start()
        loop(g * R, (g + 1) * R, lambda e: launch(attbuf, at_send, at_recv, e, *reach(e), None, (False, True)))

        if hub:
            for k in range(2):
                @pl.when(is_hub & (g < G - 1) & (g * 2 + 1 + k < pieces))
                def _():
                    w_relay(g * 2 + 1 + k)

    if hub:
        @pl.when(is_hub)
        def _():
            w_relay(0)

    loop(0, G, head_step)
    each_own_weights(lambda copy: copy.wait())

    far = jnp.where(z < S // 2, S - 1 - z, z)

    def slot_step(k):
        if hub:
            @pl.when(is_hub & (k == min(1, side_lag)))
            def _():
                loop(min(pieces, 2 * G - 1), pieces, w_relay)

        with jax.named_scope("arelay"):
            for rightward in (False, True):
                @pl.when((k >= side_lag) & ((inward > 0) if rightward else (inward < 0)))
                def _():
                    relay_slot(jnp.maximum(k - side_lag, 0), rightward)

            for rightward in (False, True):
                @pl.when((inward < 0) if rightward else (inward > 0))
                def _():
                    relay_slot(k, rightward)

        if hub:
            @pl.when(is_hub & (k == extra_slot))
            def _():
                with jax.named_scope("wother"):
                    for t in range(1, Y):
                        loop(0, pieces, lambda i: w_pass(i, 1, (y + t) % Y).wait_recv())

        split = hub and G > 1
        last_slot = far * E - 1

        def unsplit(act):
            def guarded(zb):
                if split:
                    @pl.when(jnp.logical_not(is_hub & (k == last_slot) & (zb == z + inward * far)))
                    def _():
                        act(zb)
                else:
                    act(zb)

            return guarded

        by_slot(k, unsplit(multiply_all), 0)
        if hub:
            by_slot(k, unsplit(multiply_extra), extra_slot)
        if split:
            @pl.when(is_hub & (k == last_slot - R))
            def _():
                multiply_most(z + inward * far)

            @pl.when(is_hub & (k == last_slot))
            def _():
                multiply_last(z + inward * far)

        def reduce_soon(zb):
            @pl.when(jnp.logical_not(is_hub & (zb == z + inward)))
            def _():
                reduce_all(zb)

        @pl.when(k > 1)
        def _():
            by_slot(k - 2, reduce_soon if hub else reduce_all, self_done)

        if hub:
            @pl.when(is_hub & (k == E + side_lag))
            def _():
                reduce_all(z + inward)

    slots = jnp.maximum(far * E, (S - 1 - far) * E + side_lag)
    loop(0, slots, slot_step)
    if hub:
        reduce_extra(z)
        reduce_extra(z + inward)
        reduce_extra(z - inward)
    loop(slots - 2, slots, lambda k: by_slot(k, reduce_all, self_done))
    if hub:
        def reduce_far(d):
            for way in (-inward, inward):
                zb = z + way * d

                @pl.when((zb >= 0) & (zb < S))
                def _():
                    reduce_extra(jnp.clip(zb, 0, S - 1))

        loop(2, S - 1, reduce_far)

    def finish(i):
        zs, g = i // G, i % G
        drain(kvbuf, kv_send, kv_recv, zs, g, 0, S - 1)

    def finish_att(i):
        zs, e = i // E, i % E
        drain(attbuf, at_send, at_recv, zs, e, *reach(e))

    with jax.named_scope("drain"):
        loop(0, S * G, finish)
        loop(0, S * E, finish_att)

    def each_result(u, act):
        def one(s):
            act(s * H + h, u)

        loop(0, n // H, one)

    def finish_x(u):
        def finish_one(t):
            @pl.when(t % H != h)
            def _():
                x_copy(t, u).wait_send()

        @pl.when(((u < Q) & ((inner | outer) if near else inner)) | ((u >= Q) & is_hub))
        def _():
            loop(0, n, finish_one)
            if hub and near:
                @pl.when(outer)
                def _():
                    each_result(u, lambda t, u: merge_copy(t, u).wait_send())

    def finish_results(u):
        home, slot, q = place_of(u)

        def finish_one(t, u):
            @pl.when(jnp.logical_not((t == own) & (home == h)))
            def _():
                result_copy(t, u).wait_send()

        @pl.when(inner & ((u < Q) | is_hub))
        def _():
            each_result(u, finish_one)

    units = Q * (2 if hub else 1)
    loop(0, units, finish_x)

    if hub:
        @pl.when(outer)
        def _():
            loop(0, pieces, lambda i: w_out(i).wait_send())

        @pl.when(is_hub)
        def _():
            for k in range(1, Y):
                loop(0, pieces, lambda i: w_pass(i, k, y).wait_send())
    loop(0, G, lambda g: att_copy(g).wait())

    res_copy.wait()
    squares = jnp.zeros((rows, 1), jnp.float32)
    for b in range(blocks):
        block = h * blocks + b
        source = block // C
        if hub:
            source = jnp.clip(source, 1, S - 2)
        made_here = (source == z) & (block % C == c) & (own % H == h)
        for q in range(Q):
            @pl.when(jnp.logical_not(made_here))
            def _():
                with jax.named_scope(f"final{b}_{q}"):
                    pltpu.make_async_remote_copy(
                        src_ref=obuf.at[0, 0], dst_ref=retbuf.at[b, q],
                        send_sem=ret_send.at[0, 0], recv_sem=ret_recv.at[b, q],
                        device_id={"heads": (h + 1) % H}, device_id_type=MESH,
                    ).wait_recv()
            where = slice((b * Q + q) * thin, (b * Q + q + 1) * thin)
            hidden = (res_ref[:, where].astype(jnp.float32) + retbuf[b, q].astype(jnp.float32)).astype(jnp.bfloat16)
            hidden_out[:, where] = hidden
            wide = hidden.astype(jnp.float32)
            squares = squares + jnp.sum(wide * wide, axis=-1, keepdims=True)

    ebuf[h] = jnp.broadcast_to(squares, (rows, 128))
    hidden_copy = pltpu.make_async_copy(hidden_out, hidden_hbm, out_sem.at[0])

    def share(k, side):
        other = (h + k) % H if side == 0 else (h + H - k) % H
        return pltpu.make_async_remote_copy(
            src_ref=ebuf.at[h], dst_ref=ebuf.at[h if side == 0 else other],
            send_sem=en_send.at[k], recv_sem=en_recv.at[h if side == 0 else other],
            device_id={"heads": (h + k) % H}, device_id_type=MESH,
        )

    for k in range(1, H):
        share(k, 0).start()
    hidden_copy.start()
    gain_copy.wait()
    loop(0, units, finish_results)
    with jax.named_scope("energy"):
        for k in range(1, H):
            share(k, 1).wait_recv()
    energy = ebuf[0]
    for k in range(1, H):
        energy = energy + ebuf[k]
    inverse = lax.rsqrt(energy[:, 0:1] / (H * res_ref.shape[1]) + 1e-06)
    for b in range(blocks):
        where = slice(b * Q * thin, (b + 1) * Q * thin)
        normed_out[:, where] = (
            hidden_out[:, where].astype(jnp.float32) * inverse * gain_ref[:, where]
        ).astype(jnp.bfloat16)
    normed_copy = pltpu.make_async_copy(normed_out, normed_hbm, out_sem.at[1])
    normed_copy.start()
    for k in range(1, H):
        share(k, 0).wait_send()
    hidden_copy.wait()
    normed_copy.wait()


def deliver(*refs):
    count = len(refs) // 3
    given, out, held = refs[:count], refs[count:2 * count], refs[2 * count:3 * count]
    sem = refs[3 * count]
    fetch = [pltpu.make_async_copy(given[i], held[i], sem.at[0, i]) for i in range(count)]
    store = [pltpu.make_async_copy(held[i], out[i], sem.at[1, i]) for i in range(count)]
    for copy in fetch:
        copy.start()
    for i in range(count):
        fetch[i].wait()
        store[i].start()
    for copy in store:
        copy.wait()


def shards(dims, queries, keys, values, half_order, frame_lengths, out_proj, residual_in, norm_gain):
    S, C, H, Y = dims
    n = S * C
    rows = queries.shape[0]
    G = keys.shape[1] // HEAD_WIDTH
    width = queries.shape[1] // G
    deep, cols = out_proj.shape
    hub = S >= 4
    Q = 2 if cols % 512 == 0 else 1
    NJ = 4
    near = G // 2
    thin = cols // Q
    U = Q * (2 if hub else 1)
    E = G * (2 if width // HEAD_WIDTH % 4 == 0 else 1)
    hbm = pl.BlockSpec(memory_space=pltpu.HBM)
    vmem = pl.BlockSpec(memory_space=pltpu.VMEM)
    dma = pltpu.SemaphoreType.DMA
    bf16, f32 = jnp.bfloat16, jnp.float32
    made = pl.pallas_call(
        functools.partial(kernel, (S, C, H, G, Y, Q, NJ, hub, near)),
        out_shape=(
            jax.ShapeDtypeStruct(queries.shape, bf16),
            jax.ShapeDtypeStruct(residual_in.shape, bf16),
            jax.ShapeDtypeStruct(residual_in.shape, bf16),
        ),
        in_specs=[hbm, hbm, hbm, hbm, hbm, hbm, hbm, hbm],
        out_specs=(hbm, hbm, hbm),
        scratch_shapes=[
            pltpu.SMEM(half_order.shape, jnp.int32),
            pltpu.SMEM(frame_lengths.shape, jnp.int32),
            pltpu.VMEM(residual_in.shape, bf16),
            pltpu.VMEM(residual_in.shape, bf16),
            pltpu.VMEM((U, C * rows, thin), f32),
            pltpu.VMEM((n, G, 2, rows, HEAD_WIDTH), bf16),
            pltpu.VMEM((n, G, rows, width), bf16),
            pltpu.VMEM((Q, deep, thin), bf16),
            pltpu.VMEM((Q, (G - near) * width, thin), bf16),
            pltpu.VMEM(queries.shape, bf16),
            pltpu.VMEM(residual_in.shape, bf16),
            pltpu.VMEM((1, norm_gain.shape[0]), f32),
            pltpu.VMEM((rows, n * rows), f32),
            pltpu.VMEM((U, n, rows, thin), bf16),
            pltpu.VMEM((U, n // H, H, rows, thin), bf16),
            pltpu.VMEM((U, n // H, rows, thin), bf16),
            pltpu.VMEM((Q, n // H, rows, thin), bf16),
            pltpu.VMEM((n // H, Q, rows, thin), bf16),
            pltpu.VMEM((H, rows, 128), f32),
            dma((5 + Q,)),
            dma((2 + G,)),
            dma((G, 2)),
            dma((3, S, G)),
            dma((n, G)),
            dma((3, S, E)),
            dma((n, E)),
            dma((U, n)),
            dma((U, n // H, H)),
            dma((U, n // H)),
            dma((n // H, Q)),
            dma((Q, n // H)),
            dma((Q * NJ,)),
            dma((Y, Q * NJ)),
            dma((max(Y - 1, 1), Q * NJ)),
            dma((H,)),
            dma((H,)),
        ],
        compiler_params=pltpu.CompilerParams(
            collective_id=0, has_side_effects=True, vmem_limit_bytes=60 * 1024 * 1024
        ),
    )(half_order, frame_lengths, queries, keys, values, out_proj, residual_in, norm_gain[None, :])
    return pl.pallas_call(
        deliver,
        out_shape=tuple(jax.ShapeDtypeStruct(a.shape, bf16) for a in made),
        in_specs=[hbm] * 3,
        out_specs=(hbm,) * 3,
        scratch_shapes=[pltpu.VMEM(a.shape, bf16) for a in made] + [dma((2, 3))],
    )(*made)


def solution(mesh):
    dims = (mesh.shape["seq"], mesh.shape["sub"], mesh.shape["heads"], mesh.shape["groups"])
    token = P(("groups", "seq", "sub"), "heads")
    in_specs = (
        token, token, token, P("groups"), P("groups"),
        P("heads", ("seq", "sub")), token, P("heads"),
    )
    return jax.shard_map(
        functools.partial(shards, dims), mesh=mesh, in_specs=in_specs,
        out_specs=(token, token, token), check_vma=False,
    )
```

```python
import functools
import math

import jax
import jax.numpy as jnp
from jax import lax
from jax.experimental import pallas as pl
from jax.experimental.pallas import tpu as pltpu
from jax.sharding import PartitionSpec as P

HEAD_WIDTH = 128
MESH = pl.DeviceIdType.MESH


def loop(low, high, body):
    def step(i, carry):
        body(i)
        return carry

    lax.fori_loop(low, high, step, 0)


def kernel(dims, order_hbm, frames_hbm, q_hbm, k_hbm, v_hbm, proj_hbm, res_hbm, gain_hbm,
           att_hbm, hidden_hbm, normed_hbm,
           order_ref, frames_ref, hidden_out, normed_out, kvbuf, attbuf, wall, wext, q_ref, res_ref, gain_ref, bias, pbuf, xbuf, obuf, mbuf, retbuf, ebuf,
           in_sem, out_sem, kv_in, kv_send, kv_recv, at_send, at_recv, at_part, x_send, x_recv, ret_send, ret_recv,
           m_recv, w_send, w_recv, wy_recv, wf_send, en_send, en_recv):
    S, C, H, G, Y, Q, NJ, hub, near = dims
    n = S * C
    blocks = n // H
    rows = q_ref.shape[0]
    width = q_ref.shape[1] // G
    deep, thin = wall.shape[1], wall.shape[2]
    total = n * rows
    part_rows = wext.shape[1] // Y
    piece_rows = part_rows // NJ
    pieces = Q * NJ
    steps = width // HEAD_WIDTH
    pack = 2 if steps % 2 == 0 else 1
    steps = steps // pack
    span = pack * HEAD_WIDTH
    pace, lead = min(3, steps), min(1, steps - 1)
    R = 2 if steps % 2 == 0 else 1
    E = G * R
    cut_width = width // R
    side_lag = min(2, E - 1)
    mid = min(2, pieces - NJ)
    self_done = E // 2
    extra_slot = min(side_lag + 4, E - 1)
    y, z = lax.axis_index("groups"), lax.axis_index("seq")
    c, h = lax.axis_index("sub"), lax.axis_index("heads")
    own = z * C + c
    inner = (z >= 1) & (z <= S - 2) if hub else (z >= 0)
    outer = jnp.logical_not(inner)
    is_hub = (z == 1) | (z == S - 2)
    edge = jnp.where(z < S // 2, 0, S - 1)
    hub_of_edge = jnp.where(z < S // 2, 1, S - 2)
    inward = jnp.where(z < S // 2, 1, -1)

    def is_edge(zs):
        return (zs == 0) | (zs == S - 1)

    def rows_piece(e):
        rest = jnp.maximum(e - near * R, 0)
        first = e < near * R
        return jnp.where(first, e % R, rest // (G - near)), jnp.where(first, e // R, near + rest % (G - near))

    def part_of(e):
        return jnp.maximum(e - near * R, 0) // (G - near)

    def reach(e):
        if not hub:
            return 0, S - 1
        wide = e < near * R
        return jnp.where(wide, 0, 1), jnp.where(wide, S - 1, S - 2)

    kv_copies = []
    for g in range(G):
        part = slice(g * HEAD_WIDTH, (g + 1) * HEAD_WIDTH)
        kv_copies.append(pltpu.make_async_copy(k_hbm.at[:, part], kvbuf.at[own, g, 0], kv_in.at[g, 0]))
        kv_copies.append(pltpu.make_async_copy(v_hbm.at[:, part], kvbuf.at[own, g, 1], kv_in.at[g, 1]))
    for copy in kv_copies:
        copy.start()
    table_copies = [
        pltpu.make_async_copy(order_hbm, order_ref, in_sem.at[3]),
        pltpu.make_async_copy(frames_hbm, frames_ref, in_sem.at[4]),
    ]
    for copy in table_copies:
        copy.start()
    q_copy = pltpu.make_async_copy(q_hbm, q_ref, in_sem.at[0])
    q_copy.start()
    barrier = pltpu.get_barrier_semaphore()

    def greet(t):
        other = lax.rem(own * H + h + t, n * H)
        place = other // H
        pl.semaphore_signal(
            barrier, inc=1,
            device_id={"seq": place // C, "sub": place % C, "heads": other % H},
            device_id_type=MESH,
        )

    loop(1, n * H, greet)
    greeted = n * H - 1
    if hub:
        for k in range(1, Y):
            pl.semaphore_signal(barrier, inc=1, device_id={"groups": (y + k) % Y}, device_id_type=MESH)
        greeted += Y - 1

    res_copy = pltpu.make_async_copy(res_hbm, res_ref, in_sem.at[1])
    res_copy.start()
    gain_copy = pltpu.make_async_copy(gain_hbm, gain_ref, in_sem.at[2])
    gain_copy.start()

    def own_weights(q, depth):
        return pltpu.make_async_copy(
            proj_hbm.at[:depth, q * thin:(q + 1) * thin], wall.at[q, :depth, :], in_sem.at[5 + q]
        )

    def each_own_weights(act):
        @pl.when(inner)
        def _():
            for q in range(Q):
                act(own_weights(q, deep))

        if hub and near:
            @pl.when(outer)
            def _():
                for q in range(Q):
                    act(own_weights(q, near * width))

    each_own_weights(lambda copy: copy.start())
    with jax.named_scope("kvload"):
        for copy in kv_copies:
            copy.wait()
    with jax.named_scope("barrier"):
        pl.semaphore_wait(barrier, greeted)

    def hop(buf, send, recv, side, zs, cs, g, cut=None, by_rows=False):
        target = ({"seq": jnp.minimum(z + 1, S - 1)}, {"seq": jnp.maximum(z - 1, 0)}, {"sub": (c + 1) % C})[side]
        index = zs * C + cs
        if side < 2:
            landing = recv.at[zs, g]
        elif buf is kvbuf:
            landing = recv.at[S, g]
        else:
            landing = at_part.at[zs, part_of(g)]
        if buf is kvbuf:
            block = buf.at[index, g]
        elif by_rows:
            size = rows // R
            band, group = rows_piece(g)
            block = buf.at[index, group, pl.ds(pl.multiple_of(band * size, size), size), :]
        else:
            if cut is None:
                cut = pl.ds(pl.multiple_of(g % R * cut_width, HEAD_WIDTH), cut_width)
            block = buf.at[index, g // R, :, cut]
        return pltpu.make_async_remote_copy(
            src_ref=block,
            dst_ref=block,
            send_sem=send.at[side, zs],
            recv_sem=landing,
            device_id=target,
            device_id_type=MESH,
        )

    def begin(buf, send, recv, side, zs, cs, g):
        if buf is kvbuf or not hub:
            hop(buf, send, recv, side, zs, cs, g).start()
        else:
            @pl.when(is_edge(zs))
            def _():
                hop(buf, send, recv, side, zs, cs, g, by_rows=True).start()

            @pl.when(jnp.logical_not(is_edge(zs)))
            def _():
                hop(buf, send, recv, side, zs, cs, g).start()

    def launch(buf, send, recv, g, lo, hi, cut=None, ways=(True, True), by_rows=False):
        inward_too, edgeward_too = ways

        @pl.when((z + 1 <= hi) & jnp.where(inward > 0, inward_too, edgeward_too))
        def _():
            hop(buf, send, recv, 0, z, c, g, cut, by_rows).start()

        @pl.when((z - 1 >= lo) & jnp.where(inward < 0, inward_too, edgeward_too))
        def _():
            hop(buf, send, recv, 1, z, c, g, cut, by_rows).start()

        if C > 1 and inward_too:
            @pl.when((z >= lo) & (z <= hi))
            def _():
                hop(buf, send, recv, 2, z, c, g, cut, by_rows).start()

    def relay_right(buf, send, recv, d, g, lo, hi):
        @pl.when((z - d >= 0) & (z >= lo) & (z <= hi))
        def _():
            hop(buf, send, recv, 0, z - d, c, g).wait_recv()

            @pl.when(z + 1 <= hi)
            def _():
                begin(buf, send, recv, 0, z - d, c, g)

            if C > 1:
                begin(buf, send, recv, 2, z - d, c, g)

    def relay_left(buf, send, recv, d, g, lo, hi):
        @pl.when((z + d < S) & (z >= lo) & (z <= hi))
        def _():
            hop(buf, send, recv, 1, z + d, c, g).wait_recv()

            @pl.when(z - 1 >= lo)
            def _():
                begin(buf, send, recv, 1, z + d, c, g)

            if C > 1:
                begin(buf, send, recv, 2, z + d, c, g)

    def sized(ref, send_sem, recv_sem):
        return pltpu.make_async_remote_copy(
            src_ref=ref, dst_ref=ref, send_sem=send_sem, recv_sem=recv_sem,
            device_id={"sub": (c + 1) % C}, device_id_type=MESH,
        )

    def landed(zs, part, count):
        if C > 1 and count:
            some = attbuf.at[pl.ds(0, count), 0, pl.ds(0, rows // R), :]
            sized(some, at_send.at[0, zs], at_part.at[zs, part]).wait_recv()

    def drain(buf, send, zs, kept):
        index = zs * C + c

        def done(side, cond, full):
            block = buf.at[index] if full else buf.at[index, pl.ds(0, kept)]

            @pl.when(cond)
            def _():
                sized(block, send.at[side, zs], send.at[side, zs]).wait_send()

        right, left = (zs <= z) & (z + 1 < S), (zs >= z) & (z > 0)
        if kept is None:
            done(0, right, True)
            done(1, left, True)
            if C > 1:
                done(2, z >= 0, True)
        else:
            done(0, right & (z + 1 < S - 1), True)
            done(1, left & (z > 1), True)
            if C > 1:
                done(2, inner, True)
            if kept:
                done(0, right & (z + 1 == S - 1), False)
                done(1, left & (z == 1), False)
                if C > 1:
                    done(2, outer, False)

    def w_block(i, side):
        q, j = i // NJ, i % NJ
        return q, side * part_rows + j * piece_rows

    def w_out(i):
        q, at = w_block(i, y)
        return pltpu.make_async_remote_copy(
            src_ref=proj_hbm.at[
                pl.ds(pl.multiple_of(near * width + at, piece_rows), piece_rows),
                pl.ds(pl.multiple_of(q * thin, thin), thin),
            ],
            dst_ref=wext.at[q, pl.ds(pl.multiple_of(at, piece_rows), piece_rows), :],
            send_sem=w_send.at[0], recv_sem=w_recv.at[i],
            device_id={"seq": hub_of_edge}, device_id_type=MESH,
        )

    def w_pass(i, k):
        q, at = w_block(i, y)
        block = wext.at[q, pl.ds(pl.multiple_of(at, piece_rows), piece_rows), :]
        return pltpu.make_async_remote_copy(
            src_ref=block, dst_ref=block,
            send_sem=wf_send.at[k - 1], recv_sem=wy_recv.at[Y - 1 - k, q],
            device_id={"groups": (y + k) % Y}, device_id_type=MESH,
        )

    def w_relay(i):
        with jax.named_scope("wwait"):
            w_out(i).wait_recv()
        for k in range(1, Y):
            w_pass(i, k).start()

    def w_landed(q):
        for k in range(1, Y):
            some = wext.at[q, pl.ds(0, part_rows), :]
            sized(some, wf_send.at[k - 1], wy_recv.at[k - 1, q]).wait_recv()

    def wave(s):
        @pl.when((s + 2 < G) & (inner if hub else True))
        def _():
            launch(kvbuf, kv_send, kv_recv, jnp.minimum(s + 2, G - 1), 0, S - 1)

        def either(d, ahead):
            g = s + 1 - d + ahead

            @pl.when((g >= 0) & (g < G))
            def _():
                at = jnp.clip(g, 0, G - 1)

                @pl.when((inward > 0) == (ahead > 0))
                def _():
                    relay_right(kvbuf, kv_send, kv_recv, d, at, 0, S - 1)

                @pl.when((inward < 0) == (ahead > 0))
                def _():
                    relay_left(kvbuf, kv_send, kv_recv, d, at, 0, S - 1)

        def one(d):
            either(d, 1)
            either(d, 0)

        with jax.named_scope("wave"):
            loop(1, S, one)

    def kv_partner(g):
        with jax.named_scope("kvpartner"):
            if C > 1:
                sized(kvbuf.at[pl.ds(0, S), g], kv_send.at[0, 0], kv_recv.at[S, g]).wait_recv()

    loop(0, min(2, G), lambda g: launch(kvbuf, kv_send, kv_recv, g, 0, S - 1))
    if hub:
        @pl.when(outer)
        def _():
            loop(min(2, G), G, lambda g: launch(kvbuf, kv_send, kv_recv, g, 0, S - 1))
            loop(0, NJ, lambda i: w_out(i).start())

    for copy in table_copies:
        copy.wait()
    half_rows = total // order_ref.shape[0]
    per_device = rows // half_rows
    lane = lax.broadcasted_iota(jnp.int32, (1, total), 1)
    key_pos = jnp.zeros((1, total), jnp.int32)
    for t in range(order_ref.shape[0]):
        inside = (lane >= t * half_rows) & (lane < (t + 1) * half_rows)
        key_pos = jnp.where(inside, lane + (order_ref[t] - t) * half_rows, key_pos)
    line = lax.broadcasted_iota(jnp.int32, (rows, 1), 0)
    row_pos = jnp.zeros((rows, 1), jnp.int32)
    for t in range(per_device):
        inside = (line >= t * half_rows) & (line < (t + 1) * half_rows)
        row_pos = jnp.where(inside, line + (order_ref[own * per_device + t] - t) * half_rows, row_pos)
    limit = jnp.zeros((rows, 1), jnp.int32)
    first = jnp.int32(0)
    for f in range(frames_ref.shape[0]):
        limit = limit + jnp.where(first <= row_pos, frames_ref[f], 0)
        first = first + frames_ref[f]
    bias[...] = jnp.where(key_pos < limit, 0.0, -1e30)

    factor = HEAD_WIDTH ** (-0.5) * math.log2(math.e)

    def attention(g):
        kv_partner(g)
        key = kvbuf[:, g, 0].reshape(total, HEAD_WIDTH)
        value = kvbuf[:, g, 1].reshape(total, HEAD_WIDTH)

        def few_heads(b):
            at = pl.multiple_of(g * width + b * span, span)
            q = q_ref[:, pl.ds(at, span)]
            q = jnp.concatenate(
                [q[:, k * HEAD_WIDTH:(k + 1) * HEAD_WIDTH] for k in range(pack)], axis=0
            )
            s = lax.dot_general(q, key, (((1,), (1,)), ((), ())), preferred_element_type=jnp.float32)
            s = (s.reshape(pack, rows, total) + bias[...][None]).reshape(pack * rows, total)
            top = jnp.max(s, axis=-1, keepdims=True)
            w = jnp.exp2((s - top) * factor)
            amount = jnp.sum(w, axis=-1, keepdims=True)
            o = jnp.dot(w.astype(jnp.bfloat16), value, preferred_element_type=jnp.float32)
            o = (o / amount).astype(jnp.bfloat16)
            o = jnp.concatenate([o[k * rows:(k + 1) * rows] for k in range(pack)], axis=1)
            cut = pl.ds(pl.multiple_of(b * span, span), span)
            attbuf[own, g, :, cut] = o
            e = g * R + b * R // steps

            @pl.when(inner)
            def _():
                launch(attbuf, at_send, at_recv, e, *reach(e), cut, (True, False))

            turn = g * steps + b - lead

            @pl.when((turn >= 0) & (turn % pace == 0) & (turn // pace < G - 1))
            def _():
                wave(S - 1 + turn // pace)

        loop(0, steps, few_heads)

    def span_of(part):
        if part is None:
            return slice(0, rows)
        size = rows // R
        return slice(part * size, (part + 1) * size)

    extra_slots = max(1, C // H)

    def x_slot(t, part):
        return t // H if not part else n // H + (part - 1) * extra_slots + t // H % extra_slots

    def x_copy(t, u, part=None):
        where = span_of(part)
        return pltpu.make_async_remote_copy(
            src_ref=pbuf.at[u, t, where],
            dst_ref=xbuf.at[u, t // H, h, where],
            send_sem=x_send.at[u],
            recv_sem=x_recv.at[u, x_slot(t, part), jnp.minimum((h - t % H - 1) % H, max(H - 2, 0))],
            device_id={"heads": t % H},
            device_id_type=MESH,
        )

    def multiply(zb, u, weights, g0, g1, base, part=None):
        where = span_of(part)
        tall = where.stop - where.start
        summed = jnp.zeros((C * tall, thin), jnp.float32)
        for g in range(g0, g1):
            summed = summed + jnp.dot(
                attbuf[pl.ds(zb * C, C), g, where].reshape(C * tall, width),
                weights[u % Q, (g - base) * width:(g - base + 1) * width, :],
                preferred_element_type=jnp.float32,
            )
        summed = summed.astype(jnp.bfloat16)
        for k in range(C):
            t = zb * C + k
            mine = t % H == h

            @pl.when(mine)
            def _():
                xbuf[u, t // H, h, where] = summed[k * tall:(k + 1) * tall]

            @pl.when(jnp.logical_not(mine))
            def _():
                pbuf[u, t, where] = summed[k * tall:(k + 1) * tall]
                x_copy(t, u, part).start()

    def place_of(u):
        block = jnp.where(u < Q, own, edge * C + c)
        return block // blocks, block % blocks, u % Q

    def result_copy(t, u, part=None):
        home, slot, q = place_of(u)
        where = span_of(part)
        return pltpu.make_async_remote_copy(
            src_ref=obuf.at[u, t // H, where],
            dst_ref=retbuf.at[slot, q, where],
            send_sem=ret_send.at[u],
            recv_sem=ret_recv.at[slot, q],
            device_id={"seq": t // C, "sub": t % C, "heads": home},
            device_id_type=MESH,
        )

    def merge_copy(t, u):
        return pltpu.make_async_remote_copy(
            src_ref=obuf.at[u, t // H],
            dst_ref=mbuf.at[u % Q, t // H],
            send_sem=ret_send.at[u],
            recv_sem=m_recv.at[u % Q, t // H],
            device_id={"seq": hub_of_edge},
            device_id_type=MESH,
        )

    def reduce(zb, u, part=None):
        home, slot, q = place_of(u)
        where = span_of(part)
        for k in range(C):
            t = zb * C + k

            @pl.when(t % H == h)
            def _():
                value = jnp.zeros((where.stop - where.start, thin), jnp.float32)
                for other in range(H):
                    @pl.when(other != h)
                    def _():
                        pltpu.make_async_remote_copy(
                            src_ref=pbuf.at[u, t, where], dst_ref=xbuf.at[u, t // H, other, where],
                            send_sem=x_send.at[u], recv_sem=x_recv.at[u, x_slot(t, part), jnp.minimum((other - h - 1) % H, max(H - 2, 0))],
                            device_id={"heads": (h + 1) % H}, device_id_type=MESH,
                        ).wait_recv()
                    value = value + xbuf[u, t // H, other, where].astype(jnp.float32)
                obuf[u, t // H, where] = value.astype(jnp.bfloat16)
                if hub and near:
                    @pl.when(u >= Q)
                    def _():
                        if not part:
                            merge_copy(t, u).wait_recv()
                        both = value + mbuf[q, t // H, where].astype(jnp.float32)
                        obuf[u, t // H, where] = both.astype(jnp.bfloat16)

                    @pl.when(outer)
                    def _():
                        merge_copy(t, u).start()
                here = (t == own) & (home == h)

                @pl.when(inner & here)
                def _():
                    retbuf[slot, q, where] = obuf[u, t // H, where]

                @pl.when(inner & jnp.logical_not(here))
                def _():
                    result_copy(t, u, part).start()

    def arrive(zb, parts):
        with jax.named_scope("arrive"):
            for part in parts:
                landed(zb, part, G - near + (0 if part else near * R))

    def multiply_inner(zb, part=None):
        with jax.named_scope("mult"):
            loop(0, Q, lambda u: multiply(zb, u, wall, 0, G, 0, part))

    def multiply_end(zb):
        with jax.named_scope("arrive"):
            landed(zb, 0, near * R)
        with jax.named_scope("multend"):
            loop(0, Q, lambda u: multiply(zb, u, wall, 0, near, 0))

    def multiply_all(zb):
        @pl.when(inner)
        def _():
            arrive(zb, range(R))
            multiply_inner(zb)

        if hub and near:
            @pl.when(outer)
            def _():
                multiply_end(zb)

    def multiply_extra(zb, u0=Q, u1=Q + 1, part=None):
        @pl.when(is_hub)
        def _():
            with jax.named_scope("extra"):
                loop(u0, u1, lambda u: multiply(zb, u, wext, near, G, near, part))

    def reduce_extra(zb, part=None):
        @pl.when(is_hub)
        def _():
            with jax.named_scope("reduceextra"):
                loop(Q, 2 * Q, lambda u: reduce(zb, u, part))

    def reduce_all(zb, part=None):
        with jax.named_scope("reduce"):
            @pl.when((inner | outer) if near else inner)
            def _():
                loop(0, Q, lambda u: reduce(zb, u, part))

    def by_slot(k, act, self_slot):
        def pick(which):
            since = jnp.where(which == 2, k - side_lag, k)
            d = jnp.where(which == 0, 0, since // E + 1)
            zb = z + jnp.where(which == 2, -inward, inward) * d
            due = jnp.where(which == 0, k == self_slot, (since >= 0) & (since % E == E - 1))

            @pl.when(due & (zb >= 0) & (zb < S))
            def _():
                act(jnp.clip(zb, 0, S - 1))

        loop(0, 3, pick)

    def relay_slot(k, rightward):
        d, g = k // E + 1, k % E
        move = relay_right if rightward else relay_left
        move(attbuf, at_send, at_recv, d, g, *reach(g))

    @pl.when(inward > 0)
    def _():
        relay_right(kvbuf, kv_send, kv_recv, 1, 0, 0, S - 1)

    @pl.when(inward < 0)
    def _():
        relay_left(kvbuf, kv_send, kv_recv, 1, 0, 0, S - 1)

    loop(0, S - 1, wave)
    q_copy.wait()

    def send_rows(e):
        launch(attbuf, at_send, at_recv, e, *reach(e), by_rows=True)

    def att_copy(g):
        return pltpu.make_async_copy(
            attbuf.at[own, g], att_hbm.at[:, pl.ds(pl.multiple_of(g * width, width), width)], out_sem.at[2 + g]
        )

    def head_step(g):
        with jax.named_scope("attention"):
            attention(g)
        att_copy(g).start()
        @pl.when(inner)
        def _():
            loop(g * R, (g + 1) * R, lambda e: launch(attbuf, at_send, at_recv, e, *reach(e), None, (False, True)))

        if hub:
            @pl.when(outer)
            def _():
                first = jnp.where(g < near, g * R, near * (R - 1) + g)
                loop(first, first + jnp.where(g < near, R, 1), send_rows)

            @pl.when(outer & (g == 0))
            def _():
                loop(NJ, NJ + mid, lambda i: w_out(i).start())

        if hub:
            for k in range(2):
                @pl.when(is_hub & (g < G - 1) & (g * 2 + 1 + k < NJ))
                def _():
                    w_relay(g * 2 + 1 + k)

    if hub:
        @pl.when(is_hub)
        def _():
            w_relay(0)

    loop(0, G, head_step)
    if hub:
        @pl.when(outer)
        def _():
            loop(near * (R - 1) + G, E, send_rows)
            loop(NJ + mid, pieces, lambda i: w_out(i).start())

    each_own_weights(lambda copy: copy.wait())

    far = jnp.where(z < S // 2, S - 1 - z, z)

    def slot_step(k):
        if hub:
            @pl.when(is_hub & (k == min(1, side_lag)))
            def _():
                loop(min(NJ, 2 * G - 1), NJ, w_relay)

            @pl.when(is_hub & (k == min(4, E - 1)))
            def _():
                loop(NJ, NJ + mid, w_relay)

        last_slot = far * E - 1
        late, first_late = E + side_lag + 1, NJ + mid
        if hub and Q > 1:
            @pl.when(is_hub & (k >= late) & (k < last_slot) & (k - late + first_late < pieces))
            def _():
                w_relay(k - late + first_late)

        with jax.named_scope("arelay"):
            for rightward in (False, True):
                @pl.when((k >= side_lag) & ((inward > 0) if rightward else (inward < 0)))
                def _():
                    relay_slot(jnp.maximum(k - side_lag, 0), rightward)

            for rightward in (False, True):
                @pl.when((inward < 0) if rightward else (inward > 0))
                def _():
                    relay_slot(k, rightward)

        if hub:
            @pl.when(is_hub & (k == extra_slot))
            def _():
                with jax.named_scope("wother"):
                    w_landed(0)

        far_plane = z + inward * far

        def unsplit(act, also=None):
            def guarded(zb):
                if hub:
                    skip = is_hub & (zb == far_plane)
                    if also is not None:
                        skip = skip | also(zb)

                    @pl.when(jnp.logical_not(skip))
                    def _():
                        act(zb)
                else:
                    act(zb)

            return guarded

        by_slot(k, unsplit(multiply_all), 0)
        if hub:
            by_slot(k, unsplit(multiply_extra), extra_slot)
            if Q > 1:
                @pl.when(is_hub & (k == last_slot - 1))
                def _():
                    loop(jnp.clip(first_late + last_slot - late, first_late, pieces), pieces, w_relay)
                    with jax.named_scope("wother2"):
                        loop(1, Q, w_landed)
                    for way in (0, 1, -1):
                        multiply_extra(z + inward * way, Q + 1, 2 * Q)
                    for part in range(R - 1):
                        multiply_extra(far_plane, Q + 1, 2 * Q, part)
            start = (far - 1) * E + near * R
            for part in range(R):
                @pl.when(is_hub & (k == start + (part + 1) * (G - near) - 1))
                def _():
                    arrive(far_plane, [part])
                    multiply_inner(far_plane, part)
                    multiply_extra(far_plane, part=part)
                    if Q > 1 and part == R - 1:
                        multiply_extra(far_plane, Q + 1, 2 * Q, part)

        @pl.when(k > 1)
        def _():
            by_slot(k - 2, unsplit(reduce_all, lambda zb: is_hub & (zb == z + inward)), self_done)

        if hub:
            @pl.when(is_hub & (k == E + side_lag))
            def _():
                reduce_all(z + inward)


    slots = jnp.maximum(far * E, (S - 1 - far) * E + side_lag)
    loop(0, slots, slot_step)
    def settle(zb):
        @pl.when(jnp.logical_not((is_hub & (zb == z + inward)) | (is_hub & (zb == z + inward * far))) if hub else True)
        def _():
            reduce_all(zb)

    loop(slots - 2, slots, lambda k: by_slot(k, settle, self_done))
    if hub:
        reduce_extra(z)
        reduce_extra(z + inward)
        reduce_extra(z - inward)

        @pl.when(is_hub)
        def _():
            loop(2, far, lambda d: reduce_extra(z + inward * d))
            for part in range(R):
                reduce_all(z + inward * far, part)
                reduce_extra(z + inward * far, part)

    with jax.named_scope("drain"):
        loop(0, S, lambda zs: drain(kvbuf, kv_send, zs, None))
        loop(0, S, lambda zs: drain(attbuf, at_send, zs, near if hub else None))

    units = Q * (2 if hub else 1)
    partial = n - n // H

    def working(u):
        return inner & ((u < Q) | is_hub)

    def finish_x(u):
        @pl.when((working(u) | (outer & (u < Q))) if near else working(u))
        def _():
            if partial:
                sized(pbuf.at[u, pl.ds(0, partial)], x_send.at[u], x_send.at[u]).wait_send()

        if hub and near:
            @pl.when(outer & (u < Q))
            def _():
                sized(obuf.at[u], ret_send.at[u], ret_send.at[u]).wait_send()

    def finish_results(u):
        home, slot, q = place_of(u)
        kept = (own % H == h) & (home == h)

        @pl.when(working(u) & jnp.logical_not(kept))
        def _():
            sized(obuf.at[u], ret_send.at[u], ret_send.at[u]).wait_send()

        if n // H > 1:
            @pl.when(working(u) & kept)
            def _():
                sized(obuf.at[u, pl.ds(0, n // H - 1)], ret_send.at[u], ret_send.at[u]).wait_send()

    loop(0, units, finish_x)

    if hub:
        share_rows = wext.at[:, pl.ds(0, part_rows), :]

        @pl.when(outer)
        def _():
            sized(share_rows, w_send.at[0], w_send.at[0]).wait_send()

        @pl.when(is_hub)
        def _():
            for k in range(1, Y):
                sized(share_rows, wf_send.at[k - 1], wf_send.at[k - 1]).wait_send()
    loop(0, G, lambda g: att_copy(g).wait())

    res_copy.wait()
    squares = jnp.zeros((rows, 1), jnp.float32)
    for b in range(blocks):
        block = h * blocks + b
        source = block // C
        if hub:
            source = jnp.clip(source, 1, S - 2)
        made_here = (source == z) & (block % C == c) & (own % H == h)
        for q in range(Q):
            @pl.when(jnp.logical_not(made_here))
            def _():
                with jax.named_scope(f"final{b}_{q}"):
                    pltpu.make_async_remote_copy(
                        src_ref=obuf.at[0, 0], dst_ref=retbuf.at[b, q],
                        send_sem=ret_send.at[0], recv_sem=ret_recv.at[b, q],
                        device_id={"heads": (h + 1) % H}, device_id_type=MESH,
                    ).wait_recv()
            where = slice((b * Q + q) * thin, (b * Q + q + 1) * thin)
            hidden = (res_ref[:, where].astype(jnp.float32) + retbuf[b, q].astype(jnp.float32)).astype(jnp.bfloat16)
            hidden_out[:, where] = hidden
            wide = hidden.astype(jnp.float32)
            squares = squares + jnp.sum(wide * wide, axis=-1, keepdims=True)

    ebuf[h] = jnp.broadcast_to(squares, (rows, 128))
    hidden_copy = pltpu.make_async_copy(hidden_out, hidden_hbm, out_sem.at[0])

    def share(k, side):
        other = (h + k) % H if side == 0 else (h + H - k) % H
        return pltpu.make_async_remote_copy(
            src_ref=ebuf.at[h], dst_ref=ebuf.at[h if side == 0 else other],
            send_sem=en_send.at[k], recv_sem=en_recv.at[h if side == 0 else other],
            device_id={"heads": (h + k) % H}, device_id_type=MESH,
        )

    for k in range(1, H):
        share(k, 0).start()
    hidden_copy.start()
    gain_copy.wait()
    with jax.named_scope("finres"):
        loop(0, units, finish_results)
    with jax.named_scope("energy"):
        for k in range(1, H):
            share(k, 1).wait_recv()
    energy = ebuf[0]
    for k in range(1, H):
        energy = energy + ebuf[k]
    with jax.named_scope("t_normed"):
        pass
    inverse = lax.rsqrt(energy[:, 0:1] / (H * res_ref.shape[1]) + 1e-06)
    for b in range(blocks):
        where = slice(b * Q * thin, (b + 1) * Q * thin)
        normed_out[:, where] = (
            hidden_out[:, where].astype(jnp.float32) * inverse * gain_ref[:, where]
        ).astype(jnp.bfloat16)
    normed_copy = pltpu.make_async_copy(normed_out, normed_hbm, out_sem.at[1])
    normed_copy.start()
    for k in range(1, H):
        share(k, 0).wait_send()
    with jax.named_scope("outwait"):
        hidden_copy.wait()
        normed_copy.wait()


def deliver(*refs):
    count = len(refs) // 3
    given, out, held = refs[:count], refs[count:2 * count], refs[2 * count:3 * count]
    sem = refs[3 * count]
    fetch = [pltpu.make_async_copy(given[i], held[i], sem.at[0, i]) for i in range(count)]
    store = [pltpu.make_async_copy(held[i], out[i], sem.at[1, i]) for i in range(count)]
    for copy in fetch:
        copy.start()
    for i in range(count):
        fetch[i].wait()
        store[i].start()
    for copy in store:
        copy.wait()


def shards(dims, queries, keys, values, half_order, frame_lengths, out_proj, residual_in, norm_gain):
    S, C, H, Y = dims
    n = S * C
    rows = queries.shape[0]
    G = keys.shape[1] // HEAD_WIDTH
    width = queries.shape[1] // G
    deep, cols = out_proj.shape
    hub = S >= 4
    Q = 2 if cols % 512 == 0 else 1
    NJ = 4
    near = G // 2
    thin = cols // Q
    U = Q * (2 if hub else 1)
    R = 2 if width // HEAD_WIDTH % 4 == 0 else 1
    E = G * R
    hbm = pl.BlockSpec(memory_space=pltpu.HBM)
    vmem = pl.BlockSpec(memory_space=pltpu.VMEM)
    dma = pltpu.SemaphoreType.DMA
    bf16, f32 = jnp.bfloat16, jnp.float32
    made = pl.pallas_call(
        functools.partial(kernel, (S, C, H, G, Y, Q, NJ, hub, near)),
        out_shape=(
            jax.ShapeDtypeStruct(queries.shape, bf16),
            jax.ShapeDtypeStruct(residual_in.shape, bf16),
            jax.ShapeDtypeStruct(residual_in.shape, bf16),
        ),
        in_specs=[hbm, hbm, hbm, hbm, hbm, hbm, hbm, hbm],
        out_specs=(hbm, hbm, hbm),
        scratch_shapes=[
            pltpu.SMEM(half_order.shape, jnp.int32),
            pltpu.SMEM(frame_lengths.shape, jnp.int32),
            pltpu.VMEM(residual_in.shape, bf16),
            pltpu.VMEM(residual_in.shape, bf16),
            pltpu.VMEM((n, G, 2, rows, HEAD_WIDTH), bf16),
            pltpu.VMEM((n, G, rows, width), bf16),
            pltpu.VMEM((Q, deep, thin), bf16),
            pltpu.VMEM((Q, (G - near) * width, thin), bf16),
            pltpu.VMEM(queries.shape, bf16),
            pltpu.VMEM(residual_in.shape, bf16),
            pltpu.VMEM((1, norm_gain.shape[0]), f32),
            pltpu.VMEM((rows, n * rows), f32),
            pltpu.VMEM((U, n, rows, thin), bf16),
            pltpu.VMEM((U, n // H, H, rows, thin), bf16),
            pltpu.VMEM((U, n // H, rows, thin), bf16),
            pltpu.VMEM((Q, n // H, rows, thin), bf16),
            pltpu.VMEM((n // H, Q, rows, thin), bf16),
            pltpu.VMEM((H, rows, 128), f32),
            dma((5 + Q,)),
            dma((2 + G,)),
            dma((G, 2)),
            dma((3, S)),
            dma((S + 1, G)),
            dma((3, S)),
            dma((S, E)),
            dma((S, R)),
            dma((U,)),
            dma((U, n // H + (R - 1) * max(1, C // H), max(H - 1, 1))),
            dma((U,)),
            dma((n // H, Q)),
            dma((Q, n // H)),
            dma((1,)),
            dma((Q * NJ,)),
            dma((max(Y - 1, 1), Q)),
            dma((max(Y - 1, 1),)),
            dma((H,)),
            dma((H,)),
        ],
        compiler_params=pltpu.CompilerParams(
            collective_id=0, has_side_effects=True, vmem_limit_bytes=60 * 1024 * 1024
        ),
    )(half_order, frame_lengths, queries, keys, values, out_proj, residual_in, norm_gain[None, :])
    return pl.pallas_call(
        deliver,
        out_shape=tuple(jax.ShapeDtypeStruct(a.shape, bf16) for a in made),
        in_specs=[hbm] * 3,
        out_specs=(hbm,) * 3,
        scratch_shapes=[pltpu.VMEM(a.shape, bf16) for a in made] + [dma((2, 3))],
    )(*made)


def solution(mesh):
    dims = (mesh.shape["seq"], mesh.shape["sub"], mesh.shape["heads"], mesh.shape["groups"])
    token = P(("groups", "seq", "sub"), "heads")
    in_specs = (
        token, token, token, P("groups"), P("groups"),
        P("heads", ("seq", "sub")), token, P("heads"),
    )
    return jax.shard_map(
        functools.partial(shards, dims), mesh=mesh, in_specs=in_specs,
        out_specs=(token, token, token), check_vma=False,
    )
```

```python
import functools
import math

import jax
import jax.numpy as jnp
from jax import lax
from jax.experimental import pallas as pl
from jax.experimental.pallas import tpu as pltpu
from jax.sharding import PartitionSpec as P

HEAD_WIDTH = 128
MESH = pl.DeviceIdType.MESH


def loop(low, high, body):
    def step(i, carry):
        body(i)
        return carry

    lax.fori_loop(low, high, step, 0)


def kernel(dims, order_hbm, frames_hbm, q_hbm, k_hbm, v_hbm, proj_hbm, res_hbm, gain_hbm,
           att_hbm, hidden_hbm, normed_hbm,
           order_ref, frames_ref, hidden_out, normed_out, kvbuf, attbuf, wall, wext, q_ref, res_ref, gain_ref, bias, pbuf, xbuf, obuf, mbuf, retbuf, ebuf,
           in_sem, out_sem, kv_in, kv_send, kv_recv, at_send, at_recv, at_part, x_send, x_recv, ret_send, ret_recv,
           m_recv, w_send, w_recv, wy_recv, wf_send, en_send, en_recv):
    S, C, H, G, Y, Q, NJ, hub, near = dims
    n = S * C
    blocks = n // H
    rows = q_ref.shape[0]
    width = q_ref.shape[1] // G
    deep, thin = wall.shape[1], wall.shape[2]
    total = n * rows
    part_rows = wext.shape[1] // Y
    piece_rows = part_rows // NJ
    pieces = Q * NJ
    steps = width // HEAD_WIDTH
    pack = 2 if steps % 2 == 0 else 1
    steps = steps // pack
    span = pack * HEAD_WIDTH
    pace, lead = min(3, steps), min(1, steps - 1)
    R = 2 if steps % 2 == 0 else 1
    E = G * R
    cut_width = width // R
    side_lag = min(5, E - 1)
    mid = min(2, pieces - NJ)
    self_done = E // 2
    extra_slot = min(side_lag + 4, E - 1)
    y, z = lax.axis_index("groups"), lax.axis_index("seq")
    c, h = lax.axis_index("sub"), lax.axis_index("heads")
    own = z * C + c
    inner = (z >= 1) & (z <= S - 2) if hub else (z >= 0)
    outer = jnp.logical_not(inner)
    is_hub = (z == 1) | (z == S - 2)
    edge = jnp.where(z < S // 2, 0, S - 1)
    hub_of_edge = jnp.where(z < S // 2, 1, S - 2)
    inward = jnp.where(z < S // 2, 1, -1)

    def is_edge(zs):
        return (zs == 0) | (zs == S - 1)

    def rows_piece(e):
        rest = jnp.maximum(e - near * R, 0)
        first = e < near * R
        return jnp.where(first, e % R, rest // (G - near)), jnp.where(first, e // R, near + rest % (G - near))

    def part_of(e):
        return jnp.maximum(e - near * R, 0) // (G - near)

    def reach(e):
        if not hub:
            return 0, S - 1
        wide = e < near * R
        return jnp.where(wide, 0, 1), jnp.where(wide, S - 1, S - 2)

    kv_copies = []
    for g in range(G):
        part = slice(g * HEAD_WIDTH, (g + 1) * HEAD_WIDTH)
        kv_copies.append(pltpu.make_async_copy(k_hbm.at[:, part], kvbuf.at[own, g, 0], kv_in.at[g, 0]))
        kv_copies.append(pltpu.make_async_copy(v_hbm.at[:, part], kvbuf.at[own, g, 1], kv_in.at[g, 1]))
    for copy in kv_copies:
        copy.start()
    table_copies = [
        pltpu.make_async_copy(order_hbm, order_ref, in_sem.at[3]),
        pltpu.make_async_copy(frames_hbm, frames_ref, in_sem.at[4]),
    ]
    for copy in table_copies:
        copy.start()
    q_copy = pltpu.make_async_copy(q_hbm, q_ref, in_sem.at[0])
    q_copy.start()
    barrier = pltpu.get_barrier_semaphore()

    def greet(t):
        other = lax.rem(own * H + h + t, n * H)
        place = other // H
        pl.semaphore_signal(
            barrier, inc=1,
            device_id={"seq": place // C, "sub": place % C, "heads": other % H},
            device_id_type=MESH,
        )

    loop(1, n * H, greet)
    greeted = n * H - 1
    if hub:
        for k in range(1, Y):
            pl.semaphore_signal(barrier, inc=1, device_id={"groups": (y + k) % Y}, device_id_type=MESH)
        greeted += Y - 1

    res_copy = pltpu.make_async_copy(res_hbm, res_ref, in_sem.at[1])
    res_copy.start()
    gain_copy = pltpu.make_async_copy(gain_hbm, gain_ref, in_sem.at[2])
    gain_copy.start()

    def own_weights(q, depth):
        return pltpu.make_async_copy(
            proj_hbm.at[:depth, q * thin:(q + 1) * thin], wall.at[q, :depth, :], in_sem.at[5 + q]
        )

    def each_own_weights(act):
        @pl.when(inner)
        def _():
            for q in range(Q):
                act(own_weights(q, deep))

        if hub and near:
            @pl.when(outer)
            def _():
                for q in range(Q):
                    act(own_weights(q, near * width))

    each_own_weights(lambda copy: copy.start())
    with jax.named_scope("kvload"):
        for copy in kv_copies:
            copy.wait()
    with jax.named_scope("barrier"):
        pl.semaphore_wait(barrier, greeted)

    def hop(buf, send, recv, side, zs, cs, g, cut=None, by_rows=False):
        target = ({"seq": jnp.minimum(z + 1, S - 1)}, {"seq": jnp.maximum(z - 1, 0)}, {"sub": (c + 1) % C})[side]
        index = zs * C + cs
        if side < 2:
            landing = recv.at[zs, g]
        elif buf is kvbuf:
            landing = recv.at[S, g]
        else:
            landing = at_part.at[zs, part_of(g)]
        if buf is kvbuf:
            block = buf.at[index, g]
        elif by_rows:
            size = rows // R
            band, group = rows_piece(g)
            block = buf.at[index, group, pl.ds(pl.multiple_of(band * size, size), size), :]
        else:
            if cut is None:
                cut = pl.ds(pl.multiple_of(g % R * cut_width, HEAD_WIDTH), cut_width)
            block = buf.at[index, g // R, :, cut]
        return pltpu.make_async_remote_copy(
            src_ref=block,
            dst_ref=block,
            send_sem=send.at[side, zs],
            recv_sem=landing,
            device_id=target,
            device_id_type=MESH,
        )

    def begin(buf, send, recv, side, zs, cs, g):
        if buf is kvbuf or not hub:
            hop(buf, send, recv, side, zs, cs, g).start()
        else:
            @pl.when(is_edge(zs))
            def _():
                hop(buf, send, recv, side, zs, cs, g, by_rows=True).start()

            @pl.when(jnp.logical_not(is_edge(zs)))
            def _():
                hop(buf, send, recv, side, zs, cs, g).start()

    def launch(buf, send, recv, g, lo, hi, cut=None, ways=(True, True), by_rows=False):
        inward_too, edgeward_too = ways

        @pl.when((z + 1 <= hi) & jnp.where(inward > 0, inward_too, edgeward_too))
        def _():
            hop(buf, send, recv, 0, z, c, g, cut, by_rows).start()

        @pl.when((z - 1 >= lo) & jnp.where(inward < 0, inward_too, edgeward_too))
        def _():
            hop(buf, send, recv, 1, z, c, g, cut, by_rows).start()

        if C > 1 and inward_too:
            @pl.when((z >= lo) & (z <= hi))
            def _():
                hop(buf, send, recv, 2, z, c, g, cut, by_rows).start()

    def relay_right(buf, send, recv, d, g, lo, hi):
        @pl.when((z - d >= 0) & (z >= lo) & (z <= hi))
        def _():
            hop(buf, send, recv, 0, z - d, c, g).wait_recv()

            @pl.when(z + 1 <= hi)
            def _():
                begin(buf, send, recv, 0, z - d, c, g)

            if C > 1:
                begin(buf, send, recv, 2, z - d, c, g)

    def relay_left(buf, send, recv, d, g, lo, hi):
        @pl.when((z + d < S) & (z >= lo) & (z <= hi))
        def _():
            hop(buf, send, recv, 1, z + d, c, g).wait_recv()

            @pl.when(z - 1 >= lo)
            def _():
                begin(buf, send, recv, 1, z + d, c, g)

            if C > 1:
                begin(buf, send, recv, 2, z + d, c, g)

    def sized(ref, send_sem, recv_sem):
        return pltpu.make_async_remote_copy(
            src_ref=ref, dst_ref=ref, send_sem=send_sem, recv_sem=recv_sem,
            device_id={"sub": (c + 1) % C}, device_id_type=MESH,
        )

    def landed(zs, part, count):
        if C > 1 and count:
            some = attbuf.at[pl.ds(0, count), 0, pl.ds(0, rows // R), :]
            sized(some, at_send.at[0, zs], at_part.at[zs, part]).wait_recv()

    def drain(buf, send, zs, kept):
        index = zs * C + c

        def done(side, cond, full):
            block = buf.at[index] if full else buf.at[index, pl.ds(0, kept)]

            @pl.when(cond)
            def _():
                sized(block, send.at[side, zs], send.at[side, zs]).wait_send()

        right, left = (zs <= z) & (z + 1 < S), (zs >= z) & (z > 0)
        if kept is None:
            done(0, right, True)
            done(1, left, True)
            if C > 1:
                done(2, z >= 0, True)
        else:
            done(0, right & (z + 1 < S - 1), True)
            done(1, left & (z > 1), True)
            if C > 1:
                done(2, inner, True)
            if kept:
                done(0, right & (z + 1 == S - 1), False)
                done(1, left & (z == 1), False)
                if C > 1:
                    done(2, outer, False)

    def w_block(i, side):
        q, j = i // NJ, i % NJ
        return q, side * part_rows + j * piece_rows

    def w_out(i):
        q, at = w_block(i, y)
        return pltpu.make_async_remote_copy(
            src_ref=proj_hbm.at[
                pl.ds(pl.multiple_of(near * width + at, piece_rows), piece_rows),
                pl.ds(pl.multiple_of(q * thin, thin), thin),
            ],
            dst_ref=wext.at[q, pl.ds(pl.multiple_of(at, piece_rows), piece_rows), :],
            send_sem=w_send.at[0], recv_sem=w_recv.at[i],
            device_id={"seq": hub_of_edge}, device_id_type=MESH,
        )

    def w_pass(i, k):
        q, at = w_block(i, y)
        block = wext.at[q, pl.ds(pl.multiple_of(at, piece_rows), piece_rows), :]
        return pltpu.make_async_remote_copy(
            src_ref=block, dst_ref=block,
            send_sem=wf_send.at[k - 1], recv_sem=wy_recv.at[Y - 1 - k, q],
            device_id={"groups": (y + k) % Y}, device_id_type=MESH,
        )

    def w_relay(i):
        with jax.named_scope("wwait"):
            w_out(i).wait_recv()
        for k in range(1, Y):
            w_pass(i, k).start()

    def w_landed(q):
        for k in range(1, Y):
            some = wext.at[q, pl.ds(0, part_rows), :]
            sized(some, wf_send.at[k - 1], wy_recv.at[k - 1, q]).wait_recv()

    def wave(s):
        @pl.when((s + 2 < G) & (inner if hub else True))
        def _():
            launch(kvbuf, kv_send, kv_recv, jnp.minimum(s + 2, G - 1), 0, S - 1)

        def either(d, ahead):
            g = s + 1 - d + ahead

            @pl.when((g >= 0) & (g < G))
            def _():
                at = jnp.clip(g, 0, G - 1)

                @pl.when((inward > 0) == (ahead > 0))
                def _():
                    relay_right(kvbuf, kv_send, kv_recv, d, at, 0, S - 1)

                @pl.when((inward < 0) == (ahead > 0))
                def _():
                    relay_left(kvbuf, kv_send, kv_recv, d, at, 0, S - 1)

        def one(d):
            either(d, 1)
            either(d, 0)

        with jax.named_scope("wave"):
            loop(1, S, one)

    def kv_partner(g):
        with jax.named_scope("kvpartner"):
            if C > 1:
                sized(kvbuf.at[pl.ds(0, S), g], kv_send.at[0, 0], kv_recv.at[S, g]).wait_recv()

    loop(0, min(2, G), lambda g: launch(kvbuf, kv_send, kv_recv, g, 0, S - 1))
    if hub:
        @pl.when(outer)
        def _():
            loop(min(2, G), G, lambda g: launch(kvbuf, kv_send, kv_recv, g, 0, S - 1))
            loop(0, NJ, lambda i: w_out(i).start())

    for copy in table_copies:
        copy.wait()
    half_rows = total // order_ref.shape[0]
    per_device = rows // half_rows
    lane = lax.broadcasted_iota(jnp.int32, (1, total), 1)
    key_pos = jnp.zeros((1, total), jnp.int32)
    for t in range(order_ref.shape[0]):
        inside = (lane >= t * half_rows) & (lane < (t + 1) * half_rows)
        key_pos = jnp.where(inside, lane + (order_ref[t] - t) * half_rows, key_pos)
    line = lax.broadcasted_iota(jnp.int32, (rows, 1), 0)
    row_pos = jnp.zeros((rows, 1), jnp.int32)
    for t in range(per_device):
        inside = (line >= t * half_rows) & (line < (t + 1) * half_rows)
        row_pos = jnp.where(inside, line + (order_ref[own * per_device + t] - t) * half_rows, row_pos)
    limit = jnp.zeros((rows, 1), jnp.int32)
    first = jnp.int32(0)
    for f in range(frames_ref.shape[0]):
        limit = limit + jnp.where(first <= row_pos, frames_ref[f], 0)
        first = first + frames_ref[f]
    bias[...] = jnp.where(key_pos < limit, 0.0, -1e30)

    factor = HEAD_WIDTH ** (-0.5) * math.log2(math.e)

    def attention(g):
        kv_partner(g)
        key = kvbuf[:, g, 0].reshape(total, HEAD_WIDTH)
        value = kvbuf[:, g, 1].reshape(total, HEAD_WIDTH)

        def few_heads(b):
            at = pl.multiple_of(g * width + b * span, span)
            q = q_ref[:, pl.ds(at, span)]
            q = jnp.concatenate(
                [q[:, k * HEAD_WIDTH:(k + 1) * HEAD_WIDTH] for k in range(pack)], axis=0
            )
            s = lax.dot_general(q, key, (((1,), (1,)), ((), ())), preferred_element_type=jnp.float32)
            s = (s.reshape(pack, rows, total) + bias[...][None]).reshape(pack * rows, total)
            top = jnp.max(s, axis=-1, keepdims=True)
            w = jnp.exp2((s - top) * factor)
            amount = jnp.sum(w, axis=-1, keepdims=True)
            o = jnp.dot(w.astype(jnp.bfloat16), value, preferred_element_type=jnp.float32)
            o = (o / amount).astype(jnp.bfloat16)
            o = jnp.concatenate([o[k * rows:(k + 1) * rows] for k in range(pack)], axis=1)
            cut = pl.ds(pl.multiple_of(b * span, span), span)
            attbuf[own, g, :, cut] = o
            e = g * R + b * R // steps

            @pl.when(inner)
            def _():
                launch(attbuf, at_send, at_recv, e, *reach(e), cut, (True, False))

            turn = g * steps + b - lead

            @pl.when((turn >= 0) & (turn % pace == 0) & (turn // pace < G - 1))
            def _():
                wave(S - 1 + turn // pace)

        loop(0, steps, few_heads)

    def span_of(part):
        if part is None:
            return slice(0, rows)
        size = rows // R
        return slice(part * size, (part + 1) * size)

    extra_slots = max(1, C // H)

    def x_slot(t, part):
        return t // H if not part else n // H + (part - 1) * extra_slots + t // H % extra_slots

    def x_copy(t, u, part=None):
        where = span_of(part)
        return pltpu.make_async_remote_copy(
            src_ref=pbuf.at[u, t, where],
            dst_ref=xbuf.at[u, t // H, h, where],
            send_sem=x_send.at[u],
            recv_sem=x_recv.at[u, x_slot(t, part), jnp.minimum((h - t % H - 1) % H, max(H - 2, 0))],
            device_id={"heads": t % H},
            device_id_type=MESH,
        )

    def multiply(zb, u, weights, g0, g1, base, part=None):
        where = span_of(part)
        tall = where.stop - where.start
        summed = jnp.zeros((C * tall, thin), jnp.float32)
        for g in range(g0, g1):
            summed = summed + jnp.dot(
                attbuf[pl.ds(zb * C, C), g, where].reshape(C * tall, width),
                weights[u % Q, (g - base) * width:(g - base + 1) * width, :],
                preferred_element_type=jnp.float32,
            )
        summed = summed.astype(jnp.bfloat16)
        for k in range(C):
            t = zb * C + k
            mine = t % H == h

            @pl.when(mine)
            def _():
                xbuf[u, t // H, h, where] = summed[k * tall:(k + 1) * tall]

            @pl.when(jnp.logical_not(mine))
            def _():
                pbuf[u, t, where] = summed[k * tall:(k + 1) * tall]
                x_copy(t, u, part).start()

    def place_of(u):
        block = jnp.where(u < Q, own, edge * C + c)
        return block // blocks, block % blocks, u % Q

    def result_copy(t, u, part=None):
        home, slot, q = place_of(u)
        where = span_of(part)
        return pltpu.make_async_remote_copy(
            src_ref=obuf.at[u, t // H, where],
            dst_ref=retbuf.at[slot, q, where],
            send_sem=ret_send.at[u],
            recv_sem=ret_recv.at[slot, q],
            device_id={"seq": t // C, "sub": t % C, "heads": home},
            device_id_type=MESH,
        )

    def merge_copy(t, u):
        return pltpu.make_async_remote_copy(
            src_ref=obuf.at[u, t // H],
            dst_ref=mbuf.at[u % Q, t // H],
            send_sem=ret_send.at[u],
            recv_sem=m_recv.at[u % Q, t // H],
            device_id={"seq": hub_of_edge},
            device_id_type=MESH,
        )

    def reduce(zb, u, part=None):
        home, slot, q = place_of(u)
        where = span_of(part)
        for k in range(C):
            t = zb * C + k

            @pl.when(t % H == h)
            def _():
                value = jnp.zeros((where.stop - where.start, thin), jnp.float32)
                for other in range(H):
                    @pl.when(other != h)
                    def _():
                        pltpu.make_async_remote_copy(
                            src_ref=pbuf.at[u, t, where], dst_ref=xbuf.at[u, t // H, other, where],
                            send_sem=x_send.at[u], recv_sem=x_recv.at[u, x_slot(t, part), jnp.minimum((other - h - 1) % H, max(H - 2, 0))],
                            device_id={"heads": (h + 1) % H}, device_id_type=MESH,
                        ).wait_recv()
                    value = value + xbuf[u, t // H, other, where].astype(jnp.float32)
                obuf[u, t // H, where] = value.astype(jnp.bfloat16)
                if hub and near:
                    @pl.when(u >= Q)
                    def _():
                        if not part:
                            merge_copy(t, u).wait_recv()
                        both = value + mbuf[q, t // H, where].astype(jnp.float32)
                        obuf[u, t // H, where] = both.astype(jnp.bfloat16)

                    @pl.when(outer)
                    def _():
                        merge_copy(t, u).start()
                here = (t == own) & (home == h)

                @pl.when(inner & here)
                def _():
                    retbuf[slot, q, where] = obuf[u, t // H, where]

                @pl.when(inner & jnp.logical_not(here))
                def _():
                    result_copy(t, u, part).start()

    def arrive(zb, parts):
        with jax.named_scope("arrive"):
            for part in parts:
                landed(zb, part, G - near + (0 if part else near * R))

    def multiply_inner(zb, part=None):
        with jax.named_scope("mult"):
            loop(0, Q, lambda u: multiply(zb, u, wall, 0, G, 0, part))

    def multiply_end(zb):
        with jax.named_scope("arrive"):
            landed(zb, 0, near * R)
        with jax.named_scope("multend"):
            loop(0, Q, lambda u: multiply(zb, u, wall, 0, near, 0))

    def multiply_all(zb):
        @pl.when(inner)
        def _():
            arrive(zb, range(R))
            multiply_inner(zb)

        if hub and near:
            @pl.when(outer)
            def _():
                multiply_end(zb)

    def multiply_extra(zb, u0=Q, u1=Q + 1, part=None):
        @pl.when(is_hub)
        def _():
            with jax.named_scope("extra"):
                loop(u0, u1, lambda u: multiply(zb, u, wext, near, G, near, part))

    def reduce_extra(zb, part=None, q0=0, q1=Q):
        @pl.when(is_hub)
        def _():
            with jax.named_scope("reduceextra"):
                loop(Q + q0, Q + q1, lambda u: reduce(zb, u, part))

    def reduce_all(zb, part=None):
        with jax.named_scope("reduce"):
            @pl.when((inner | outer) if near else inner)
            def _():
                loop(0, Q, lambda u: reduce(zb, u, part))

    def by_slot(k, act, self_slot):
        def pick(which):
            since = jnp.where(which == 2, k - side_lag, k)
            d = jnp.where(which == 0, 0, since // E + 1)
            zb = z + jnp.where(which == 2, -inward, inward) * d
            due = jnp.where(which == 0, k == self_slot, (since >= 0) & (since % E == E - 1))

            @pl.when(due & (zb >= 0) & (zb < S))
            def _():
                act(jnp.clip(zb, 0, S - 1))

        loop(0, 3, pick)

    def relay_slot(k, rightward):
        d, g = k // E + 1, k % E
        move = relay_right if rightward else relay_left
        move(attbuf, at_send, at_recv, d, g, *reach(g))

    @pl.when(inward > 0)
    def _():
        relay_right(kvbuf, kv_send, kv_recv, 1, 0, 0, S - 1)

    @pl.when(inward < 0)
    def _():
        relay_left(kvbuf, kv_send, kv_recv, 1, 0, 0, S - 1)

    loop(0, S - 1, wave)
    q_copy.wait()

    def send_rows(e):
        launch(attbuf, at_send, at_recv, e, *reach(e), by_rows=True)

    def att_copy(g):
        return pltpu.make_async_copy(
            attbuf.at[own, g], att_hbm.at[:, pl.ds(pl.multiple_of(g * width, width), width)], out_sem.at[2 + g]
        )

    def head_step(g):
        with jax.named_scope("attention"):
            attention(g)
        att_copy(g).start()
        @pl.when(inner)
        def _():
            loop(g * R, (g + 1) * R, lambda e: launch(attbuf, at_send, at_recv, e, *reach(e), None, (False, True)))

        if hub:
            @pl.when(outer)
            def _():
                first = jnp.where(g < near, g * R, near * (R - 1) + g)
                loop(first, first + jnp.where(g < near, R, 1), send_rows)

            @pl.when(outer & (g == 0))
            def _():
                loop(NJ, NJ + mid, lambda i: w_out(i).start())

        if hub:
            for k in range(2):
                @pl.when(is_hub & (g < G - 1) & (g * 2 + 1 + k < NJ))
                def _():
                    w_relay(g * 2 + 1 + k)

    if hub:
        @pl.when(is_hub)
        def _():
            w_relay(0)

    loop(0, G, head_step)
    if hub:
        @pl.when(outer)
        def _():
            loop(near * (R - 1) + G, E, send_rows)
            loop(NJ + mid, pieces, lambda i: w_out(i).start())

    each_own_weights(lambda copy: copy.wait())

    far = jnp.where(z < S // 2, S - 1 - z, z)

    def slot_step(k):
        if hub:
            @pl.when(is_hub & (k == min(1, side_lag)))
            def _():
                loop(min(NJ, 2 * G - 1), NJ, w_relay)

            @pl.when(is_hub & (k == min(4, E - 1)))
            def _():
                loop(NJ, NJ + mid, w_relay)

        last_slot = far * E - 1
        late, first_late = E + side_lag, NJ + mid
        if hub and Q > 1:
            @pl.when(is_hub & (k >= late) & (k < last_slot) & (k - late + first_late < pieces))
            def _():
                w_relay(k - late + first_late)

        if hub:
            @pl.when(is_hub & (k == last_slot))
            def _():
                for part in range(R - 1):
                    reduce_all(z + inward * far, part)
                reduce_extra(z - inward, None, 0, 1)

        with jax.named_scope("arelay"):
            for rightward in (False, True):
                @pl.when((k >= side_lag) & ((inward > 0) if rightward else (inward < 0)))
                def _():
                    relay_slot(jnp.maximum(k - side_lag, 0), rightward)

            for rightward in (False, True):
                @pl.when((inward < 0) if rightward else (inward > 0))
                def _():
                    relay_slot(k, rightward)

        if hub:
            @pl.when(is_hub & (k == extra_slot))
            def _():
                with jax.named_scope("wother"):
                    w_landed(0)

        far_plane = z + inward * far

        def unsplit(act, also=None):
            def guarded(zb):
                if hub:
                    skip = is_hub & (zb == far_plane)
                    if also is not None:
                        skip = skip | also(zb)

                    @pl.when(jnp.logical_not(skip))
                    def _():
                        act(zb)
                else:
                    act(zb)

            return guarded

        by_slot(k, unsplit(multiply_all), 0)
        if hub:
            by_slot(k, unsplit(multiply_extra), extra_slot)
            if Q > 1:
                @pl.when(is_hub & (k == last_slot))
                def _():
                    loop(jnp.clip(first_late + last_slot - late, first_late, pieces), pieces, w_relay)
            start = (far - 1) * E + near * R
            for part in range(R):
                @pl.when(is_hub & (k == start + (part + 1) * (G - near) - 1))
                def _():
                    arrive(far_plane, [part])
                    multiply_inner(far_plane, part)
                    multiply_extra(far_plane, part=part)
                    if Q > 1 and part == R - 1:
                        with jax.named_scope("wother2"):
                            loop(1, Q, w_landed)
                        for other in range(R):
                            multiply_extra(far_plane, Q + 1, 2 * Q, other)
                        for way in (1, -1, 0):
                            multiply_extra(z + inward * way, Q + 1, 2 * Q)

        @pl.when(k > 1)
        def _():
            by_slot(k - 2, unsplit(reduce_all, lambda zb: is_hub & (zb == z + inward)), self_done)

        if hub:
            @pl.when(is_hub & (k == E + side_lag))
            def _():
                reduce_all(z + inward)


    slots = jnp.maximum(far * E, (S - 1 - far) * E + side_lag)
    loop(0, slots, slot_step)
    def settle(zb):
        @pl.when(jnp.logical_not((is_hub & (zb == z + inward)) | (is_hub & (zb == z + inward * far))) if hub else True)
        def _():
            reduce_all(zb)

    loop(slots - 2, slots, lambda k: by_slot(k, settle, self_done))
    if hub:
        last_plane = z + inward * far

        @pl.when(is_hub)
        def _():
            for part in range(R - 1):
                reduce_extra(last_plane, part, 0, 1)
            reduce_all(last_plane, R - 1)
            reduce_extra(last_plane, R - 1, 0, 1)
            reduce_extra(z + inward, None, 0, 1)
            reduce_extra(z, None, 0, 1)
            for part in range(R):
                reduce_extra(last_plane, part, 1)
            for way in (1, -1, 0):
                reduce_extra(z + inward * way, None, 1)
            loop(2, far, lambda d: reduce_extra(z + inward * d))

    with jax.named_scope("drain"):
        loop(0, S, lambda zs: drain(kvbuf, kv_send, zs, None))
        loop(0, S, lambda zs: drain(attbuf, at_send, zs, near if hub else None))

    units = Q * (2 if hub else 1)
    partial = n - n // H

    def working(u):
        return inner & ((u < Q) | is_hub)

    def finish_x(u):
        @pl.when((working(u) | (outer & (u < Q))) if near else working(u))
        def _():
            if partial:
                sized(pbuf.at[u, pl.ds(0, partial)], x_send.at[u], x_send.at[u]).wait_send()

        if hub and near:
            @pl.when(outer & (u < Q))
            def _():
                sized(obuf.at[u], ret_send.at[u], ret_send.at[u]).wait_send()

    def finish_results(u):
        home, slot, q = place_of(u)
        kept = (own % H == h) & (home == h)

        @pl.when(working(u) & jnp.logical_not(kept))
        def _():
            sized(obuf.at[u], ret_send.at[u], ret_send.at[u]).wait_send()

        if n // H > 1:
            @pl.when(working(u) & kept)
            def _():
                sized(obuf.at[u, pl.ds(0, n // H - 1)], ret_send.at[u], ret_send.at[u]).wait_send()

    loop(0, units, finish_x)

    if hub:
        share_rows = wext.at[:, pl.ds(0, part_rows), :]

        @pl.when(outer)
        def _():
            sized(share_rows, w_send.at[0], w_send.at[0]).wait_send()

        @pl.when(is_hub)
        def _():
            for k in range(1, Y):
                sized(share_rows, wf_send.at[k - 1], wf_send.at[k - 1]).wait_send()
    loop(0, G, lambda g: att_copy(g).wait())

    res_copy.wait()
    squares = jnp.zeros((rows, 1), jnp.float32)
    shift = jnp.where(h < H // 2, blocks // 2, 0)
    for i in range(blocks):
        b = (i + shift) % blocks
        block = h * blocks + b
        source = block // C
        if hub:
            source = jnp.clip(source, 1, S - 2)
        made_here = (source == z) & (block % C == c) & (own % H == h)
        for q in range(Q):
            @pl.when(jnp.logical_not(made_here))
            def _():
                with jax.named_scope(f"final{i}_{q}"):
                    sized(retbuf.at[b, q], ret_send.at[0], ret_recv.at[b, q]).wait_recv()
            where = pl.ds(pl.multiple_of((b * Q + q) * thin, thin), thin)
            hidden = (res_ref[:, where].astype(jnp.float32) + retbuf[b, q].astype(jnp.float32)).astype(jnp.bfloat16)
            hidden_out[:, where] = hidden
            wide = hidden.astype(jnp.float32)
            squares = squares + jnp.sum(wide * wide, axis=-1, keepdims=True)

    ebuf[h] = jnp.transpose(jnp.broadcast_to(squares, (rows, 128)))[0:8]
    hidden_copy = pltpu.make_async_copy(hidden_out, hidden_hbm, out_sem.at[0])

    def share(k, side):
        other = (h + k) % H if side == 0 else (h + H - k) % H
        return pltpu.make_async_remote_copy(
            src_ref=ebuf.at[h], dst_ref=ebuf.at[h if side == 0 else other],
            send_sem=en_send.at[k], recv_sem=en_recv.at[h if side == 0 else other],
            device_id={"heads": (h + k) % H}, device_id_type=MESH,
        )

    for k in range(1, H):
        share(k, 0).start()
    hidden_copy.start()
    gain_copy.wait()
    with jax.named_scope("finres"):
        loop(0, units, finish_results)
    with jax.named_scope("energy"):
        for k in range(1, H):
            share(k, 1).wait_recv()
    energy = ebuf[0]
    for k in range(1, H):
        energy = energy + ebuf[k]
    inverse = lax.rsqrt(energy / (H * res_ref.shape[1]) + 1e-06)
    inverse = jnp.transpose(jnp.broadcast_to(inverse[0:1], (128, rows)))[:, 0:1]
    for b in range(blocks):
        where = slice(b * Q * thin, (b + 1) * Q * thin)
        normed_out[:, where] = (
            hidden_out[:, where].astype(jnp.float32) * inverse * gain_ref[:, where]
        ).astype(jnp.bfloat16)
    normed_copy = pltpu.make_async_copy(normed_out, normed_hbm, out_sem.at[1])
    normed_copy.start()
    for k in range(1, H):
        share(k, 0).wait_send()
    with jax.named_scope("outwait"):
        hidden_copy.wait()
        normed_copy.wait()


def deliver(*refs):
    count = len(refs) // 3
    given, out, held = refs[:count], refs[count:2 * count], refs[2 * count:3 * count]
    sem = refs[3 * count]
    fetch = [pltpu.make_async_copy(given[i], held[i], sem.at[0, i]) for i in range(count)]
    store = [pltpu.make_async_copy(held[i], out[i], sem.at[1, i]) for i in range(count)]
    for copy in fetch:
        copy.start()
    for i in range(count):
        fetch[i].wait()
        store[i].start()
    for copy in store:
        copy.wait()


def shards(dims, queries, keys, values, half_order, frame_lengths, out_proj, residual_in, norm_gain):
    S, C, H, Y = dims
    n = S * C
    rows = queries.shape[0]
    G = keys.shape[1] // HEAD_WIDTH
    width = queries.shape[1] // G
    deep, cols = out_proj.shape
    hub = S >= 4
    Q = 2 if cols % 512 == 0 else 1
    NJ = 4
    near = G // 2
    thin = cols // Q
    U = Q * (2 if hub else 1)
    R = 2 if width // HEAD_WIDTH % 4 == 0 else 1
    E = G * R
    hbm = pl.BlockSpec(memory_space=pltpu.HBM)
    vmem = pl.BlockSpec(memory_space=pltpu.VMEM)
    dma = pltpu.SemaphoreType.DMA
    bf16, f32 = jnp.bfloat16, jnp.float32
    made = pl.pallas_call(
        functools.partial(kernel, (S, C, H, G, Y, Q, NJ, hub, near)),
        out_shape=(
            jax.ShapeDtypeStruct(queries.shape, bf16),
            jax.ShapeDtypeStruct(residual_in.shape, bf16),
            jax.ShapeDtypeStruct(residual_in.shape, bf16),
        ),
        in_specs=[hbm, hbm, hbm, hbm, hbm, hbm, hbm, hbm],
        out_specs=(hbm, hbm, hbm),
        scratch_shapes=[
            pltpu.SMEM(half_order.shape, jnp.int32),
            pltpu.SMEM(frame_lengths.shape, jnp.int32),
            pltpu.VMEM(residual_in.shape, bf16),
            pltpu.VMEM(residual_in.shape, bf16),
            pltpu.VMEM((n, G, 2, rows, HEAD_WIDTH), bf16),
            pltpu.VMEM((n, G, rows, width), bf16),
            pltpu.VMEM((Q, deep, thin), bf16),
            pltpu.VMEM((Q, (G - near) * width, thin), bf16),
            pltpu.VMEM(queries.shape, bf16),
            pltpu.VMEM(residual_in.shape, bf16),
            pltpu.VMEM((1, norm_gain.shape[0]), f32),
            pltpu.VMEM((rows, n * rows), f32),
            pltpu.VMEM((U, n, rows, thin), bf16),
            pltpu.VMEM((U, n // H, H, rows, thin), bf16),
            pltpu.VMEM((U, n // H, rows, thin), bf16),
            pltpu.VMEM((Q, n // H, rows, thin), bf16),
            pltpu.VMEM((n // H, Q, rows, thin), bf16),
            pltpu.VMEM((H, 8, rows), f32),
            dma((5 + Q,)),
            dma((2 + G,)),
            dma((G, 2)),
            dma((3, S)),
            dma((S + 1, G)),
            dma((3, S)),
            dma((S, E)),
            dma((S, R)),
            dma((U,)),
            dma((U, n // H + (R - 1) * max(1, C // H), max(H - 1, 1))),
            dma((U,)),
            dma((n // H, Q)),
            dma((Q, n // H)),
            dma((1,)),
            dma((Q * NJ,)),
            dma((max(Y - 1, 1), Q)),
            dma((max(Y - 1, 1),)),
            dma((H,)),
            dma((H,)),
        ],
        compiler_params=pltpu.CompilerParams(
            collective_id=0, has_side_effects=True, vmem_limit_bytes=60 * 1024 * 1024
        ),
    )(half_order, frame_lengths, queries, keys, values, out_proj, residual_in, norm_gain[None, :])
    return pl.pallas_call(
        deliver,
        out_shape=tuple(jax.ShapeDtypeStruct(a.shape, bf16) for a in made),
        in_specs=[hbm] * 3,
        out_specs=(hbm,) * 3,
        scratch_shapes=[pltpu.VMEM(a.shape, bf16) for a in made] + [dma((2, 3))],
    )(*made)


def solution(mesh):
    dims = (mesh.shape["seq"], mesh.shape["sub"], mesh.shape["heads"], mesh.shape["groups"])
    token = P(("groups", "seq", "sub"), "heads")
    in_specs = (
        token, token, token, P("groups"), P("groups"),
        P("heads", ("seq", "sub")), token, P("heads"),
    )
    return jax.shard_map(
        functools.partial(shards, dims), mesh=mesh, in_specs=in_specs,
        out_specs=(token, token, token), check_vma=False,
    )
```

```python
import functools
import math

import jax
import jax.numpy as jnp
from jax import lax
from jax.experimental import pallas as pl
from jax.experimental.pallas import tpu as pltpu
from jax.sharding import PartitionSpec as P

HEAD_WIDTH = 128
MESH = pl.DeviceIdType.MESH


def loop(low, high, body):
    def step(i, carry):
        body(i)
        return carry

    lax.fori_loop(low, high, step, 0)


def kernel(dims, order_hbm, frames_hbm, q_hbm, k_hbm, v_hbm, proj_hbm, res_hbm, gain_hbm,
           att_hbm, hidden_hbm, normed_hbm,
           order_ref, frames_ref, hidden_out, normed_out, kvbuf, attbuf, wall, wext, q_ref, res_ref, gain_ref, bias, pbuf, xbuf, obuf, mbuf, retbuf, ebuf,
           in_sem, out_sem, kv_in, kv_send, kv_recv, at_send, at_recv, at_part, x_send, x_recv, ret_send, ret_recv,
           m_recv, w_send, w_recv, wy_recv, wf_send, en_send, en_recv):
    S, C, H, G, Y, Q, NJ, hub, near = dims
    n = S * C
    blocks = n // H
    rows = q_ref.shape[0]
    width = q_ref.shape[1] // G
    deep, thin = wall.shape[1], wall.shape[2]
    total = n * rows
    part_rows = wext.shape[1] // Y
    piece_rows = part_rows // NJ
    pieces = Q * NJ
    steps = width // HEAD_WIDTH
    pack = 2 if steps % 2 == 0 else 1
    steps = steps // pack
    span = pack * HEAD_WIDTH
    pace, lead = min(3, steps), min(1, steps - 1)
    R = 2 if steps % 2 == 0 else 1
    E = G * R
    cut_width = width // R
    side_lag = min(5, E - 1)
    mid = min(2, pieces - NJ)
    self_done = E // 2
    extra_slot = min(side_lag + 4, E - 1)
    y, z = lax.axis_index("groups"), lax.axis_index("seq")
    c, h = lax.axis_index("sub"), lax.axis_index("heads")
    own = z * C + c
    inner = (z >= 1) & (z <= S - 2) if hub else (z >= 0)
    outer = jnp.logical_not(inner)
    is_hub = (z == 1) | (z == S - 2)
    edge = jnp.where(z < S // 2, 0, S - 1)
    hub_of_edge = jnp.where(z < S // 2, 1, S - 2)
    inward = jnp.where(z < S // 2, 1, -1)

    def is_edge(zs):
        return (zs == 0) | (zs == S - 1)

    def rows_piece(e):
        rest = jnp.maximum(e - near * R, 0)
        first = e < near * R
        return jnp.where(first, e % R, rest // (G - near)), jnp.where(first, e // R, near + rest % (G - near))

    def part_of(e):
        return jnp.maximum(e - near * R, 0) // (G - near)

    def reach(e):
        if not hub:
            return 0, S - 1
        wide = e < near * R
        return jnp.where(wide, 0, 1), jnp.where(wide, S - 1, S - 2)

    kv_copies = []
    for g in range(G):
        part = slice(g * HEAD_WIDTH, (g + 1) * HEAD_WIDTH)
        kv_copies.append(pltpu.make_async_copy(k_hbm.at[:, part], kvbuf.at[own, g, 0], kv_in.at[g, 0]))
        kv_copies.append(pltpu.make_async_copy(v_hbm.at[:, part], kvbuf.at[own, g, 1], kv_in.at[g, 1]))
    for copy in kv_copies:
        copy.start()
    table_copies = [
        pltpu.make_async_copy(order_hbm, order_ref, in_sem.at[3]),
        pltpu.make_async_copy(frames_hbm, frames_ref, in_sem.at[4]),
    ]
    for copy in table_copies:
        copy.start()
    q_copy = pltpu.make_async_copy(q_hbm, q_ref, in_sem.at[0])
    q_copy.start()
    barrier = pltpu.get_barrier_semaphore()

    def greet(t):
        other = lax.rem(own * H + h + t, n * H)
        place = other // H
        pl.semaphore_signal(
            barrier, inc=1,
            device_id={"seq": place // C, "sub": place % C, "heads": other % H},
            device_id_type=MESH,
        )

    loop(1, n * H, greet)
    greeted = n * H - 1
    if hub:
        for k in range(1, Y):
            pl.semaphore_signal(barrier, inc=1, device_id={"groups": (y + k) % Y}, device_id_type=MESH)
        greeted += Y - 1

    res_copy = pltpu.make_async_copy(res_hbm, res_ref, in_sem.at[1])
    res_copy.start()
    gain_copy = pltpu.make_async_copy(gain_hbm, gain_ref, in_sem.at[2])
    gain_copy.start()

    def own_weights(q, depth):
        return pltpu.make_async_copy(
            proj_hbm.at[:depth, q * thin:(q + 1) * thin], wall.at[q, :depth, :], in_sem.at[5 + q]
        )

    def each_own_weights(act):
        @pl.when(inner)
        def _():
            for q in range(Q):
                act(own_weights(q, deep))

        if hub and near:
            @pl.when(outer)
            def _():
                for q in range(Q):
                    act(own_weights(q, near * width))

    each_own_weights(lambda copy: copy.start())
    with jax.named_scope("kvload"):
        for copy in kv_copies:
            copy.wait()
    with jax.named_scope("barrier"):
        pl.semaphore_wait(barrier, greeted)

    def hop(buf, send, recv, side, zs, cs, g, cut=None, by_rows=False):
        target = ({"seq": jnp.minimum(z + 1, S - 1)}, {"seq": jnp.maximum(z - 1, 0)}, {"sub": (c + 1) % C})[side]
        index = zs * C + cs
        if side < 2:
            landing = recv.at[zs, g]
        elif buf is kvbuf:
            landing = recv.at[S, g]
        else:
            landing = at_part.at[zs, part_of(g)]
        if buf is kvbuf:
            block = buf.at[index, g]
        elif by_rows:
            size = rows // R
            band, group = rows_piece(g)
            block = buf.at[index, group, pl.ds(pl.multiple_of(band * size, size), size), :]
        else:
            if cut is None:
                cut = pl.ds(pl.multiple_of(g % R * cut_width, HEAD_WIDTH), cut_width)
            block = buf.at[index, g // R, :, cut]
        return pltpu.make_async_remote_copy(
            src_ref=block,
            dst_ref=block,
            send_sem=send.at[side, zs],
            recv_sem=landing,
            device_id=target,
            device_id_type=MESH,
        )

    def begin(buf, send, recv, side, zs, cs, g):
        if buf is kvbuf or not hub:
            hop(buf, send, recv, side, zs, cs, g).start()
        else:
            @pl.when(is_edge(zs))
            def _():
                hop(buf, send, recv, side, zs, cs, g, by_rows=True).start()

            @pl.when(jnp.logical_not(is_edge(zs)))
            def _():
                hop(buf, send, recv, side, zs, cs, g).start()

    def launch(buf, send, recv, g, lo, hi, cut=None, ways=(True, True), by_rows=False):
        inward_too, edgeward_too = ways

        @pl.when((z + 1 <= hi) & jnp.where(inward > 0, inward_too, edgeward_too))
        def _():
            hop(buf, send, recv, 0, z, c, g, cut, by_rows).start()

        @pl.when((z - 1 >= lo) & jnp.where(inward < 0, inward_too, edgeward_too))
        def _():
            hop(buf, send, recv, 1, z, c, g, cut, by_rows).start()

        if C > 1 and inward_too:
            @pl.when((z >= lo) & (z <= hi))
            def _():
                hop(buf, send, recv, 2, z, c, g, cut, by_rows).start()

    def relay_right(buf, send, recv, d, g, lo, hi):
        @pl.when((z - d >= 0) & (z >= lo) & (z <= hi))
        def _():
            hop(buf, send, recv, 0, z - d, c, g).wait_recv()

            @pl.when(z + 1 <= hi)
            def _():
                begin(buf, send, recv, 0, z - d, c, g)

            if C > 1:
                begin(buf, send, recv, 2, z - d, c, g)

    def relay_left(buf, send, recv, d, g, lo, hi):
        @pl.when((z + d < S) & (z >= lo) & (z <= hi))
        def _():
            hop(buf, send, recv, 1, z + d, c, g).wait_recv()

            @pl.when(z - 1 >= lo)
            def _():
                begin(buf, send, recv, 1, z + d, c, g)

            if C > 1:
                begin(buf, send, recv, 2, z + d, c, g)

    def sized(ref, send_sem, recv_sem):
        return pltpu.make_async_remote_copy(
            src_ref=ref, dst_ref=ref, send_sem=send_sem, recv_sem=recv_sem,
            device_id={"sub": (c + 1) % C}, device_id_type=MESH,
        )

    def landed(zs, part, count):
        if C > 1 and count:
            some = attbuf.at[pl.ds(0, count), 0, pl.ds(0, rows // R), :]
            sized(some, at_send.at[0, zs], at_part.at[zs, part]).wait_recv()

    def drain(buf, send, zs, kept):
        index = zs * C + c

        def done(side, cond, full):
            block = buf.at[index] if full else buf.at[index, pl.ds(0, kept)]

            @pl.when(cond)
            def _():
                sized(block, send.at[side, zs], send.at[side, zs]).wait_send()

        right, left = (zs <= z) & (z + 1 < S), (zs >= z) & (z > 0)
        if kept is None:
            done(0, right, True)
            done(1, left, True)
            if C > 1:
                done(2, z >= 0, True)
        else:
            done(0, right & (z + 1 < S - 1), True)
            done(1, left & (z > 1), True)
            if C > 1:
                done(2, inner, True)
            if kept:
                done(0, right & (z + 1 == S - 1), False)
                done(1, left & (z == 1), False)
                if C > 1:
                    done(2, outer, False)

    def w_block(i, side):
        q, j = i // NJ, i % NJ
        return q, side * part_rows + j * piece_rows

    def w_out(i):
        q, at = w_block(i, y)
        return pltpu.make_async_remote_copy(
            src_ref=proj_hbm.at[
                pl.ds(pl.multiple_of(near * width + at, piece_rows), piece_rows),
                pl.ds(pl.multiple_of(q * thin, thin), thin),
            ],
            dst_ref=wext.at[q, pl.ds(pl.multiple_of(at, piece_rows), piece_rows), :],
            send_sem=w_send.at[0], recv_sem=w_recv.at[i],
            device_id={"seq": hub_of_edge}, device_id_type=MESH,
        )

    def w_pass(i, k):
        q, at = w_block(i, y)
        block = wext.at[q, pl.ds(pl.multiple_of(at, piece_rows), piece_rows), :]
        return pltpu.make_async_remote_copy(
            src_ref=block, dst_ref=block,
            send_sem=wf_send.at[k - 1], recv_sem=wy_recv.at[Y - 1 - k, q],
            device_id={"groups": (y + k) % Y}, device_id_type=MESH,
        )

    def w_relay(i):
        with jax.named_scope("wwait"):
            w_out(i).wait_recv()
        for k in range(1, Y):
            w_pass(i, k).start()

    def w_landed(q):
        for k in range(1, Y):
            some = wext.at[q, pl.ds(0, part_rows), :]
            sized(some, wf_send.at[k - 1], wy_recv.at[k - 1, q]).wait_recv()

    def wave(s):
        @pl.when((s + 2 < G) & (inner if hub else True))
        def _():
            launch(kvbuf, kv_send, kv_recv, jnp.minimum(s + 2, G - 1), 0, S - 1)

        def either(d, ahead):
            g = s + 1 - d + ahead

            @pl.when((g >= 0) & (g < G))
            def _():
                at = jnp.clip(g, 0, G - 1)

                @pl.when((inward > 0) == (ahead > 0))
                def _():
                    relay_right(kvbuf, kv_send, kv_recv, d, at, 0, S - 1)

                @pl.when((inward < 0) == (ahead > 0))
                def _():
                    relay_left(kvbuf, kv_send, kv_recv, d, at, 0, S - 1)

        def one(d):
            either(d, 1)
            either(d, 0)

        with jax.named_scope("wave"):
            loop(1, S, one)

    def kv_partner(g):
        with jax.named_scope("kvpartner"):
            if C > 1:
                sized(kvbuf.at[pl.ds(0, S), g], kv_send.at[0, 0], kv_recv.at[S, g]).wait_recv()

    loop(0, min(2, G), lambda g: launch(kvbuf, kv_send, kv_recv, g, 0, S - 1))
    if hub:
        @pl.when(outer)
        def _():
            loop(min(2, G), G, lambda g: launch(kvbuf, kv_send, kv_recv, g, 0, S - 1))
            loop(0, NJ, lambda i: w_out(i).start())

    for copy in table_copies:
        copy.wait()
    half_rows = total // order_ref.shape[0]
    per_device = rows // half_rows
    lane = lax.broadcasted_iota(jnp.int32, (1, total), 1)
    key_pos = jnp.zeros((1, total), jnp.int32)
    for t in range(order_ref.shape[0]):
        inside = (lane >= t * half_rows) & (lane < (t + 1) * half_rows)
        key_pos = jnp.where(inside, lane + (order_ref[t] - t) * half_rows, key_pos)
    line = lax.broadcasted_iota(jnp.int32, (rows, 1), 0)
    row_pos = jnp.zeros((rows, 1), jnp.int32)
    for t in range(per_device):
        inside = (line >= t * half_rows) & (line < (t + 1) * half_rows)
        row_pos = jnp.where(inside, line + (order_ref[own * per_device + t] - t) * half_rows, row_pos)
    limit = jnp.zeros((rows, 1), jnp.int32)
    first = jnp.int32(0)
    for f in range(frames_ref.shape[0]):
        limit = limit + jnp.where(first <= row_pos, frames_ref[f], 0)
        first = first + frames_ref[f]
    bias[...] = jnp.where(key_pos < limit, 0.0, -1e30)

    factor = HEAD_WIDTH ** (-0.5) * math.log2(math.e)

    def attention(g):
        kv_partner(g)
        key = kvbuf[:, g, 0].reshape(total, HEAD_WIDTH)
        value = kvbuf[:, g, 1].reshape(total, HEAD_WIDTH)

        def few_heads(b):
            at = pl.multiple_of(g * width + b * span, span)
            q = q_ref[:, pl.ds(at, span)]
            q = jnp.concatenate(
                [q[:, k * HEAD_WIDTH:(k + 1) * HEAD_WIDTH] for k in range(pack)], axis=0
            )
            s = lax.dot_general(q, key, (((1,), (1,)), ((), ())), preferred_element_type=jnp.float32)
            s = (s.reshape(pack, rows, total) + bias[...][None]).reshape(pack * rows, total)
            top = jnp.max(s, axis=-1, keepdims=True)
            w = jnp.exp2((s - top) * factor)
            amount = jnp.sum(w, axis=-1, keepdims=True)
            o = jnp.dot(w.astype(jnp.bfloat16), value, preferred_element_type=jnp.float32)
            o = (o / amount).astype(jnp.bfloat16)
            o = jnp.concatenate([o[k * rows:(k + 1) * rows] for k in range(pack)], axis=1)
            cut = pl.ds(pl.multiple_of(b * span, span), span)
            attbuf[own, g, :, cut] = o
            e = g * R + b * R // steps

            @pl.when(inner)
            def _():
                launch(attbuf, at_send, at_recv, e, *reach(e), cut, (True, False))

            turn = g * steps + b - lead

            @pl.when((turn >= 0) & (turn % pace == 0) & (turn // pace < G - 1))
            def _():
                wave(S - 1 + turn // pace)

        loop(0, steps, few_heads)

    def span_of(part):
        if part is None:
            return slice(0, rows)
        size = rows // R
        return slice(part * size, (part + 1) * size)

    extra_slots = max(1, C // H)

    def x_slot(t, part):
        return t // H if not part else n // H + (part - 1) * extra_slots + t // H % extra_slots

    def x_copy(t, u, part=None):
        where = span_of(part)
        return pltpu.make_async_remote_copy(
            src_ref=pbuf.at[u, t, where],
            dst_ref=xbuf.at[u, t // H, h, where],
            send_sem=x_send.at[u],
            recv_sem=x_recv.at[u, x_slot(t, part), jnp.minimum((h - t % H - 1) % H, max(H - 2, 0))],
            device_id={"heads": t % H},
            device_id_type=MESH,
        )

    def multiply(zb, u, weights, g0, g1, base, part=None):
        where = span_of(part)
        tall = where.stop - where.start
        summed = jnp.zeros((C * tall, thin), jnp.float32)
        for g in range(g0, g1):
            summed = summed + jnp.dot(
                attbuf[pl.ds(zb * C, C), g, where].reshape(C * tall, width),
                weights[u % Q, (g - base) * width:(g - base + 1) * width, :],
                preferred_element_type=jnp.float32,
            )
        summed = summed.astype(jnp.bfloat16)
        for k in range(C):
            t = zb * C + k
            mine = t % H == h

            @pl.when(mine)
            def _():
                xbuf[u, t // H, h, where] = summed[k * tall:(k + 1) * tall]

            @pl.when(jnp.logical_not(mine))
            def _():
                pbuf[u, t, where] = summed[k * tall:(k + 1) * tall]
                x_copy(t, u, part).start()

    def place_of(u):
        block = jnp.where(u < Q, own, edge * C + c)
        return block // blocks, block % blocks, u % Q

    def result_copy(t, u, part=None):
        home, slot, q = place_of(u)
        where = span_of(part)
        return pltpu.make_async_remote_copy(
            src_ref=obuf.at[u, t // H, where],
            dst_ref=retbuf.at[slot, q, where],
            send_sem=ret_send.at[u],
            recv_sem=ret_recv.at[slot, q],
            device_id={"seq": t // C, "sub": t % C, "heads": home},
            device_id_type=MESH,
        )

    def merge_copy(t, u):
        return pltpu.make_async_remote_copy(
            src_ref=obuf.at[u, t // H],
            dst_ref=mbuf.at[u % Q, t // H],
            send_sem=ret_send.at[u],
            recv_sem=m_recv.at[u % Q, t // H],
            device_id={"seq": hub_of_edge},
            device_id_type=MESH,
        )

    def reduce(zb, u, part=None):
        home, slot, q = place_of(u)
        where = span_of(part)
        for k in range(C):
            t = zb * C + k

            @pl.when(t % H == h)
            def _():
                value = jnp.zeros((where.stop - where.start, thin), jnp.float32)
                for other in range(H):
                    @pl.when(other != h)
                    def _():
                        pltpu.make_async_remote_copy(
                            src_ref=pbuf.at[u, t, where], dst_ref=xbuf.at[u, t // H, other, where],
                            send_sem=x_send.at[u], recv_sem=x_recv.at[u, x_slot(t, part), jnp.minimum((other - h - 1) % H, max(H - 2, 0))],
                            device_id={"heads": (h + 1) % H}, device_id_type=MESH,
                        ).wait_recv()
                    value = value + xbuf[u, t // H, other, where].astype(jnp.float32)
                obuf[u, t // H, where] = value.astype(jnp.bfloat16)
                if hub and near:
                    @pl.when(u >= Q)
                    def _():
                        if not part:
                            merge_copy(t, u).wait_recv()
                        both = value + mbuf[q, t // H, where].astype(jnp.float32)
                        obuf[u, t // H, where] = both.astype(jnp.bfloat16)

                    @pl.when(outer)
                    def _():
                        merge_copy(t, u).start()
                here = (t == own) & (home == h)

                @pl.when(inner & here)
                def _():
                    retbuf[slot, q, where] = obuf[u, t // H, where]

                @pl.when(inner & jnp.logical_not(here))
                def _():
                    result_copy(t, u, part).start()

    def arrive(zb, parts):
        with jax.named_scope("arrive"):
            for part in parts:
                landed(zb, part, G - near + (0 if part else near * R))

    def multiply_inner(zb, part=None):
        with jax.named_scope("mult"):
            loop(0, Q, lambda u: multiply(zb, u, wall, 0, G, 0, part))

    def multiply_end(zb):
        with jax.named_scope("arrive"):
            landed(zb, 0, near * R)
        with jax.named_scope("multend"):
            loop(0, Q, lambda u: multiply(zb, u, wall, 0, near, 0))

    def multiply_all(zb):
        @pl.when(inner)
        def _():
            arrive(zb, range(R))
            multiply_inner(zb)

        if hub and near:
            @pl.when(outer)
            def _():
                multiply_end(zb)

    def multiply_extra(zb, u0=Q, u1=Q + 1, part=None):
        @pl.when(is_hub)
        def _():
            with jax.named_scope("extra"):
                loop(u0, u1, lambda u: multiply(zb, u, wext, near, G, near, part))

    def reduce_extra(zb, part=None, q0=0, q1=Q):
        @pl.when(is_hub)
        def _():
            with jax.named_scope("reduceextra"):
                loop(Q + q0, Q + q1, lambda u: reduce(zb, u, part))

    def reduce_all(zb, part=None):
        with jax.named_scope("reduce"):
            @pl.when((inner | outer) if near else inner)
            def _():
                loop(0, Q, lambda u: reduce(zb, u, part))

    def by_slot(k, act, self_slot):
        def pick(which):
            since = jnp.where(which == 2, k - side_lag, k)
            d = jnp.where(which == 0, 0, since // E + 1)
            zb = z + jnp.where(which == 2, -inward, inward) * d
            due = jnp.where(which == 0, k == self_slot, (since >= 0) & (since % E == E - 1))

            @pl.when(due & (zb >= 0) & (zb < S))
            def _():
                act(jnp.clip(zb, 0, S - 1))

        loop(0, 3, pick)

    def relay_slot(k, rightward):
        d, g = k // E + 1, k % E
        move = relay_right if rightward else relay_left
        move(attbuf, at_send, at_recv, d, g, *reach(g))

    @pl.when(inward > 0)
    def _():
        relay_right(kvbuf, kv_send, kv_recv, 1, 0, 0, S - 1)

    @pl.when(inward < 0)
    def _():
        relay_left(kvbuf, kv_send, kv_recv, 1, 0, 0, S - 1)

    loop(0, S - 1, wave)
    q_copy.wait()

    def send_rows(e):
        launch(attbuf, at_send, at_recv, e, *reach(e), by_rows=True)

    def att_copy(g):
        return pltpu.make_async_copy(
            attbuf.at[own, g], att_hbm.at[:, pl.ds(pl.multiple_of(g * width, width), width)], out_sem.at[2 + g]
        )

    def head_step(g):
        with jax.named_scope("attention"):
            attention(g)
        att_copy(g).start()
        @pl.when(inner)
        def _():
            loop(g * R, (g + 1) * R, lambda e: launch(attbuf, at_send, at_recv, e, *reach(e), None, (False, True)))

        if hub:
            @pl.when(outer)
            def _():
                first = jnp.where(g < near, g * R, near * (R - 1) + g)
                loop(first, first + jnp.where(g < near, R, 1), send_rows)

            @pl.when(outer & (g == 0))
            def _():
                loop(NJ, NJ + mid, lambda i: w_out(i).start())

        if hub:
            for k in range(2):
                @pl.when(is_hub & (g < G - 1) & (g * 2 + 1 + k < NJ))
                def _():
                    w_relay(g * 2 + 1 + k)

    if hub:
        @pl.when(is_hub)
        def _():
            w_relay(0)

    loop(0, G, head_step)
    if hub:
        @pl.when(outer)
        def _():
            loop(near * (R - 1) + G, E, send_rows)
            loop(NJ + mid, pieces, lambda i: w_out(i).start())

    each_own_weights(lambda copy: copy.wait())

    far = jnp.where(z < S // 2, S - 1 - z, z)

    def slot_step(k):
        if hub:
            @pl.when(is_hub & (k == min(1, side_lag)))
            def _():
                loop(min(NJ, 2 * G - 1), NJ, w_relay)

            @pl.when(is_hub & (k == min(4, E - 1)))
            def _():
                loop(NJ, NJ + mid, w_relay)

        last_slot = far * E - 1
        late, first_late = E + side_lag, NJ + mid
        if hub and Q > 1:
            @pl.when(is_hub & (k >= late) & (k < last_slot) & (k - late + first_late < pieces))
            def _():
                w_relay(k - late + first_late)

        if hub:
            @pl.when(is_hub & (k == last_slot))
            def _():
                reduce_all(z - inward)
                reduce_extra(z - inward, None, 0, 1)

        with jax.named_scope("arelay"):
            for rightward in (False, True):
                @pl.when((k >= side_lag) & ((inward > 0) if rightward else (inward < 0)))
                def _():
                    relay_slot(jnp.maximum(k - side_lag, 0), rightward)

            for rightward in (False, True):
                @pl.when((inward < 0) if rightward else (inward > 0))
                def _():
                    relay_slot(k, rightward)

        if hub:
            @pl.when(is_hub & (k == extra_slot))
            def _():
                with jax.named_scope("wother"):
                    w_landed(0)

        far_plane = z + inward * far

        def unsplit(act, also=None):
            def guarded(zb):
                if hub:
                    skip = is_hub & (zb == far_plane)
                    if also is not None:
                        skip = skip | also(zb)

                    @pl.when(jnp.logical_not(skip))
                    def _():
                        act(zb)
                else:
                    act(zb)

            return guarded

        by_slot(k, unsplit(multiply_all), 0)
        if hub:
            by_slot(k, unsplit(multiply_extra), extra_slot)
            if Q > 1:
                @pl.when(is_hub & (k == last_slot))
                def _():
                    loop(jnp.clip(first_late + last_slot - late, first_late, pieces), pieces, w_relay)
            start = (far - 1) * E + near * R
            for part in range(R):
                @pl.when(is_hub & (k == start + (part + 1) * (G - near) - 1))
                def _():
                    arrive(far_plane, [part])
                    multiply_inner(far_plane, part)
                    multiply_extra(far_plane, part=part)
                    if part == R - 1:
                        for other in range(R - 1):
                            reduce_all(far_plane, other)
                    if Q > 1 and part == R - 1:
                        with jax.named_scope("wother2"):
                            loop(1, Q, w_landed)
                        for other in range(R):
                            multiply_extra(far_plane, Q + 1, 2 * Q, other)
                        for way in (-1, 1, 0):
                            multiply_extra(z + inward * way, Q + 1, 2 * Q)

        @pl.when(k > 1)
        def _():
            by_slot(k - 2, unsplit(reduce_all, lambda zb: is_hub & ((zb == z + inward) | (zb == z - inward))), self_done)

        if hub:
            @pl.when(is_hub & (k == E + side_lag))
            def _():
                reduce_all(z + inward)


    slots = jnp.maximum(far * E, (S - 1 - far) * E + side_lag)
    loop(0, slots, slot_step)
    def settle(zb):
        @pl.when(jnp.logical_not(is_hub & ((zb == z + inward) | (zb == z - inward) | (zb == z + inward * far))) if hub else True)
        def _():
            reduce_all(zb)

    loop(slots - 2, slots, lambda k: by_slot(k, settle, self_done))
    if hub:
        last_plane = z + inward * far

        @pl.when(is_hub)
        def _():
            for part in range(R - 1):
                reduce_extra(last_plane, part, 0, 1)
            reduce_extra(z + inward, None, 0, 1)
            reduce_all(last_plane, R - 1)
            reduce_extra(last_plane, R - 1, 0, 1)
            reduce_extra(z, None, 0, 1)
            for part in range(R):
                reduce_extra(last_plane, part, 1)
            for way in (-1, 1, 0):
                reduce_extra(z + inward * way, None, 1)
            loop(2, far, lambda d: reduce_extra(z + inward * d))

    with jax.named_scope("drain"):
        loop(0, S, lambda zs: drain(kvbuf, kv_send, zs, None))
        loop(0, S, lambda zs: drain(attbuf, at_send, zs, near if hub else None))

    units = Q * (2 if hub else 1)
    partial = n - n // H

    def working(u):
        return inner & ((u < Q) | is_hub)

    def finish_x(u):
        @pl.when((working(u) | (outer & (u < Q))) if near else working(u))
        def _():
            if partial:
                sized(pbuf.at[u, pl.ds(0, partial)], x_send.at[u], x_send.at[u]).wait_send()

        if hub and near:
            @pl.when(outer & (u < Q))
            def _():
                sized(obuf.at[u], ret_send.at[u], ret_send.at[u]).wait_send()

    def finish_results(u):
        home, slot, q = place_of(u)
        kept = (own % H == h) & (home == h)

        @pl.when(working(u) & jnp.logical_not(kept))
        def _():
            sized(obuf.at[u], ret_send.at[u], ret_send.at[u]).wait_send()

        if n // H > 1:
            @pl.when(working(u) & kept)
            def _():
                sized(obuf.at[u, pl.ds(0, n // H - 1)], ret_send.at[u], ret_send.at[u]).wait_send()

    loop(0, units, finish_x)

    if hub:
        share_rows = wext.at[:, pl.ds(0, part_rows), :]

        @pl.when(outer)
        def _():
            sized(share_rows, w_send.at[0], w_send.at[0]).wait_send()

        @pl.when(is_hub)
        def _():
            for k in range(1, Y):
                sized(share_rows, wf_send.at[k - 1], wf_send.at[k - 1]).wait_send()
    loop(0, G, lambda g: att_copy(g).wait())

    res_copy.wait()
    squares = jnp.zeros((rows, 1), jnp.float32)
    shift = jnp.where(h < H // 2, blocks // 2, 0)
    for i in range(blocks):
        b = (i + shift) % blocks
        block = h * blocks + b
        source = block // C
        if hub:
            source = jnp.clip(source, 1, S - 2)
        made_here = (source == z) & (block % C == c) & (own % H == h)
        for q in range(Q):
            @pl.when(jnp.logical_not(made_here))
            def _():
                with jax.named_scope(f"final{i}_{q}"):
                    sized(retbuf.at[b, q], ret_send.at[0], ret_recv.at[b, q]).wait_recv()
            where = pl.ds(pl.multiple_of((b * Q + q) * thin, thin), thin)
            hidden = (res_ref[:, where].astype(jnp.float32) + retbuf[b, q].astype(jnp.float32)).astype(jnp.bfloat16)
            hidden_out[:, where] = hidden
            wide = hidden.astype(jnp.float32)
            squares = squares + jnp.sum(wide * wide, axis=-1, keepdims=True)

    ebuf[h] = jnp.transpose(jnp.broadcast_to(squares, (rows, 128)))[0:8]
    hidden_copy = pltpu.make_async_copy(hidden_out, hidden_hbm, out_sem.at[0])

    def share(k, side):
        other = (h + k) % H if side == 0 else (h + H - k) % H
        return pltpu.make_async_remote_copy(
            src_ref=ebuf.at[h], dst_ref=ebuf.at[h if side == 0 else other],
            send_sem=en_send.at[k], recv_sem=en_recv.at[h if side == 0 else other],
            device_id={"heads": (h + k) % H}, device_id_type=MESH,
        )

    for k in range(1, H):
        share(k, 0).start()
    hidden_copy.start()
    gain_copy.wait()
    with jax.named_scope("finres"):
        loop(0, units, finish_results)
    with jax.named_scope("energy"):
        for k in range(1, H):
            share(k, 1).wait_recv()
    energy = ebuf[0]
    for k in range(1, H):
        energy = energy + ebuf[k]
    inverse = lax.rsqrt(energy / (H * res_ref.shape[1]) + 1e-06)
    inverse = jnp.transpose(jnp.broadcast_to(inverse[0:1], (128, rows)))[:, 0:1]
    for b in range(blocks):
        where = slice(b * Q * thin, (b + 1) * Q * thin)
        normed_out[:, where] = (
            hidden_out[:, where].astype(jnp.float32) * inverse * gain_ref[:, where]
        ).astype(jnp.bfloat16)
    normed_copy = pltpu.make_async_copy(normed_out, normed_hbm, out_sem.at[1])
    normed_copy.start()
    for k in range(1, H):
        share(k, 0).wait_send()
    with jax.named_scope("outwait"):
        hidden_copy.wait()
        normed_copy.wait()


def deliver(*refs):
    count = len(refs) // 3
    given, out, held = refs[:count], refs[count:2 * count], refs[2 * count:3 * count]
    sem = refs[3 * count]
    pieces = []
    for i in reversed(range(count)):
        tall = given[i].shape[0]
        cuts = 4 if i == 0 and tall % 32 == 0 else 1
        pieces += [(i, pl.ds(k * (tall // cuts), tall // cuts)) for k in range(cuts)]
    fetch = [
        pltpu.make_async_copy(given[i].at[at], held[i].at[at], sem.at[0, p]) for p, (i, at) in enumerate(pieces)
    ]
    store = [
        pltpu.make_async_copy(held[i].at[at], out[i].at[at], sem.at[1, p]) for p, (i, at) in enumerate(pieces)
    ]
    for copy in fetch:
        copy.start()
    for p in range(len(pieces)):
        fetch[p].wait()
        store[p].start()
    for copy in store:
        copy.wait()


def shards(dims, queries, keys, values, half_order, frame_lengths, out_proj, residual_in, norm_gain):
    S, C, H, Y = dims
    n = S * C
    rows = queries.shape[0]
    G = keys.shape[1] // HEAD_WIDTH
    width = queries.shape[1] // G
    deep, cols = out_proj.shape
    hub = S >= 4
    Q = 2 if cols % 512 == 0 else 1
    NJ = 4
    near = G // 2
    thin = cols // Q
    U = Q * (2 if hub else 1)
    R = 2 if width // HEAD_WIDTH % 4 == 0 else 1
    E = G * R
    hbm = pl.BlockSpec(memory_space=pltpu.HBM)
    vmem = pl.BlockSpec(memory_space=pltpu.VMEM)
    dma = pltpu.SemaphoreType.DMA
    bf16, f32 = jnp.bfloat16, jnp.float32
    made = pl.pallas_call(
        functools.partial(kernel, (S, C, H, G, Y, Q, NJ, hub, near)),
        out_shape=(
            jax.ShapeDtypeStruct(queries.shape, bf16),
            jax.ShapeDtypeStruct(residual_in.shape, bf16),
            jax.ShapeDtypeStruct(residual_in.shape, bf16),
        ),
        in_specs=[hbm, hbm, hbm, hbm, hbm, hbm, hbm, hbm],
        out_specs=(hbm, hbm, hbm),
        scratch_shapes=[
            pltpu.SMEM(half_order.shape, jnp.int32),
            pltpu.SMEM(frame_lengths.shape, jnp.int32),
            pltpu.VMEM(residual_in.shape, bf16),
            pltpu.VMEM(residual_in.shape, bf16),
            pltpu.VMEM((n, G, 2, rows, HEAD_WIDTH), bf16),
            pltpu.VMEM((n, G, rows, width), bf16),
            pltpu.VMEM((Q, deep, thin), bf16),
            pltpu.VMEM((Q, (G - near) * width, thin), bf16),
            pltpu.VMEM(queries.shape, bf16),
            pltpu.VMEM(residual_in.shape, bf16),
            pltpu.VMEM((1, norm_gain.shape[0]), f32),
            pltpu.VMEM((rows, n * rows), f32),
            pltpu.VMEM((U, n, rows, thin), bf16),
            pltpu.VMEM((U, n // H, H, rows, thin), bf16),
            pltpu.VMEM((U, n // H, rows, thin), bf16),
            pltpu.VMEM((Q, n // H, rows, thin), bf16),
            pltpu.VMEM((n // H, Q, rows, thin), bf16),
            pltpu.VMEM((H, 8, rows), f32),
            dma((5 + Q,)),
            dma((2 + G,)),
            dma((G, 2)),
            dma((3, S)),
            dma((S + 1, G)),
            dma((3, S)),
            dma((S, E)),
            dma((S, R)),
            dma((U,)),
            dma((U, n // H + (R - 1) * max(1, C // H), max(H - 1, 1))),
            dma((U,)),
            dma((n // H, Q)),
            dma((Q, n // H)),
            dma((1,)),
            dma((Q * NJ,)),
            dma((max(Y - 1, 1), Q)),
            dma((max(Y - 1, 1),)),
            dma((H,)),
            dma((H,)),
        ],
        compiler_params=pltpu.CompilerParams(
            collective_id=0, has_side_effects=True, vmem_limit_bytes=60 * 1024 * 1024
        ),
    )(half_order, frame_lengths, queries, keys, values, out_proj, residual_in, norm_gain[None, :])
    return pl.pallas_call(
        deliver,
        out_shape=tuple(jax.ShapeDtypeStruct(a.shape, bf16) for a in made),
        in_specs=[hbm] * 3,
        out_specs=(hbm,) * 3,
        scratch_shapes=[pltpu.VMEM(a.shape, bf16) for a in made] + [dma((2, 6))],
    )(*made)


def solution(mesh):
    dims = (mesh.shape["seq"], mesh.shape["sub"], mesh.shape["heads"], mesh.shape["groups"])
    token = P(("groups", "seq", "sub"), "heads")
    in_specs = (
        token, token, token, P("groups"), P("groups"),
        P("heads", ("seq", "sub")), token, P("heads"),
    )
    return jax.shard_map(
        functools.partial(shards, dims), mesh=mesh, in_specs=in_specs,
        out_specs=(token, token, token), check_vma=False,
    )
```
